64 devices in a mesh: rep: 4 (over x, y), dp: 16 (over z, core).
Axes of the slice: x: 2, y: 2, z: 8, core: 2. Of those that a mesh axis runs over, the one named last changes fastest.
The devices are a block of a 4x4x8 slice.
Arguments:
- g_w_gate: bfloat16 [64, 2, 768, 1792], P(('rep', 'dp')), parts along dimension 0
- g_w_up: bfloat16 [64, 2, 768, 1792], P(('rep', 'dp')), parts along dimension 0
- g_w_down: bfloat16 [64, 2, 1792, 768], P(('rep', 'dp')), parts along dimension 0
- w_gate: bfloat16 [2, 768, 1792], replicated
- w_up: bfloat16 [2, 768, 1792], replicated
- w_down: bfloat16 [2, 1792, 768], replicated
- m_w_gate: float32 [2, 768, 1792], P(None, 'dp')
- m_w_up: float32 [2, 768, 1792], P(None, 'dp')
- m_w_down: float32 [2, 1792, 768], P(None, 'dp')
- v_w_gate: float32 [2, 768, 1792], P(None, 'dp')
- v_w_up: float32 [2, 768, 1792], P(None, 'dp')
- v_w_down: float32 [2, 1792, 768], P(None, 'dp')
Outputs:
- output 1: bfloat16 [8, 768, 1792], P('rep'), parts along dimension 0
- output 2: bfloat16 [8, 768, 1792], P('rep'), parts along dimension 0
- output 3: bfloat16 [8, 1792, 768], P('rep'), parts along dimension 0
- output 4: float32 [8, 768, 1792], P('rep', 'dp'), parts along dimension 0
- output 5: float32 [8, 768, 1792], P('rep', 'dp'), parts along dimension 0
- output 6: float32 [8, 1792, 768], P('rep', 'dp'), parts along dimension 0
- output 7: float32 [8, 768, 1792], P('rep', 'dp'), parts along dimension 0
- output 8: float32 [8, 768, 1792], P('rep', 'dp'), parts along dimension 0
- output 9: float32 [8, 1792, 768], P('rep', 'dp'), parts along dimension 0
There are 4 independent parts. The reference program is written for one: setup_inputs(seed, part) draws one part's arguments, and reference() takes and returns one part's arrays. A program takes and returns all parts, laid end to end along the dimension named above; an argument that names none is the same for every part.
All inputs are finite; a program needn't handle non-finite values.
Results may differ from the reference program's by a relative error of at most 0.022.
Values are sent between devices in bfloat16 or wider.
A program may use at most 768 MiB of HBM per device.

```python
import jax
import jax.numpy as jnp
from jax import lax

DEVICES = 16
D = 768
FF = 1792
LAYERS = 2
NAMES = ("w_gate", "w_up", "w_down")
SHAPES = {"w_gate": (LAYERS, D, FF), "w_up": (LAYERS, D, FF), "w_down": (LAYERS, FF, D)}


def setup_inputs(seed: int = 0, part: int = 0) -> dict:
    kz, *keys = jax.random.split(jax.random.key(seed), 1 + 5 * len(NAMES))
    loud = 2.0 ** jax.random.uniform(kz, (), jnp.float32, -1.0, 1.0)
    drawn = {}
    for name, key, both in zip(NAMES, keys[:3], keys[3:6], strict=True):
        own = jax.random.normal(jax.random.fold_in(key, part), (DEVICES, *SHAPES[name]), jnp.float32)
        shared = jax.random.normal(jax.random.fold_in(both, part), SHAPES[name], jnp.float32)
        drawn["g_" + name] = (loud * (0.7 * shared / DEVICES + 0.7 * own * DEVICES**-0.5)).astype(jnp.bfloat16)
    for name, key in zip(NAMES, keys[6:9], strict=True):
        drawn[name] = (jax.random.normal(key, SHAPES[name], jnp.float32) * SHAPES[name][1] ** -0.5).astype(jnp.bfloat16)
    for name, key in zip(NAMES, keys[9:12], strict=True):
        drawn["m_" + name] = loud * 0.5 * jax.random.normal(key, SHAPES[name], jnp.float32)
    for name, key in zip(NAMES, keys[12:15], strict=True):
        drawn["v_" + name] = loud * loud * jax.random.uniform(key, SHAPES[name], jnp.float32, 0.5, 1.5)
    return drawn


def adamw(w, m, v, g):
    m = 0.9 * m + 0.1 * g
    v = 0.95 * v + 0.05 * g * g
    step = m * lax.rsqrt(v + 1e-8) + 0.1 * w
    return (w - 0.02 * step).astype(jnp.bfloat16), m, v


def reference(g_w_gate, g_w_up, g_w_down, w_gate, w_up, w_down, m_w_gate, m_w_up, m_w_down, v_w_gate, v_w_up, v_w_down):
    def total(terms):
        return lax.scan(lambda so_far, term: (so_far + term.astype(jnp.float32), None), jnp.zeros(terms.shape[1:], jnp.float32), terms)[0]

    gradients = [total(terms).astype(jnp.bfloat16).astype(jnp.float32) for terms in (g_w_gate, g_w_up, g_w_down)]
    new = [
        adamw(w.astype(jnp.float32), m, v, g)
        for w, m, v, g in zip((w_gate, w_up, w_down), (m_w_gate, m_w_up, m_w_down), (v_w_gate, v_w_up, v_w_down), gradients, strict=True)
    ]
    return tuple(one[which] for which in range(3) for one in new)
```

```python
import functools

import jax
import jax.numpy as jnp
from jax import lax
from jax.experimental import pallas as pl
from jax.experimental.pallas import tpu as pltpu
from jax.sharding import PartitionSpec as P

MESH = pl.DeviceIdType.MESH
CORES = 2
AHEAD = 2
TILE = 16


def adamw(w, m, v, g):
    m = 0.9 * m + 0.1 * g
    v = 0.95 * v + 0.05 * g * g
    step = m * lax.rsqrt(v + 1e-8) + 0.1 * w
    return (w - 0.02 * step).astype(jnp.bfloat16), m, v


def kernel(n, terms, weights, m_in, v_in, new, m_out, v_out, mine, theirs, partial, own_w, sems):
    (mine_sem, give_sem, take_sem, load_sem, sum_out, sum_in, ring_out, ring_in, fwd_out, fwd_in) = sems
    chips = n // CORES
    me = lax.axis_index("dp")
    chip, core = me // CORES, me % CORES
    way = 1 - CORES * core
    other = chip * CORES + (1 - core)

    def device_at(steps, which):
        return lax.rem(chip + way * steps + chips, chips) * CORES + which

    onward, behind = device_at(1, core), device_at(-1, core)
    layers = weights[0].shape[0]
    pieces = [(i, l) for i in range(len(terms)) for l in range(layers)]
    height = [ref.shape[2] for ref in mine]

    def rows(i, device):
        return pl.ds(pl.multiple_of(device * height[i], TILE), height[i])

    def fetch(s, p):
        i, l = pieces[p]
        return pltpu.make_async_copy(terms[i].at[0, l, rows(i, device_at(-1 - s, core))], mine[i].at[s, l], mine_sem.at[s, p])

    def give(s, p):
        i, l = pieces[p]
        return pltpu.make_async_remote_copy(
            src_ref=terms[i].at[0, l, rows(i, device_at(1 + s, 1 - core))],
            dst_ref=theirs[i].at[s, l],
            send_sem=give_sem.at[s, p],
            recv_sem=take_sem.at[s, p],
            device_id={"dp": other},
            device_id_type=MESH,
        )

    def send_sum(s, p):
        i, l = pieces[p]
        return pltpu.make_async_remote_copy(
            src_ref=mine[i].at[s, l],
            dst_ref=partial[i].at[s, l],
            send_sem=sum_out.at[s, p],
            recv_sem=sum_in.at[s, p],
            device_id={"dp": onward},
            device_id_type=MESH,
        )

    def send_new(s, p):
        i, l = pieces[p]
        block = new[i].at[l, rows(i, device_at(-s, core))]
        return pltpu.make_async_remote_copy(
            src_ref=block,
            dst_ref=block,
            send_sem=ring_out.at[s, p],
            recv_sem=ring_in.at[s, p],
            device_id={"dp": onward},
            device_id_type=MESH,
        )

    def forward(s, p):
        i, l = pieces[p]
        block = new[i].at[l, rows(i, device_at(-s, core))]
        return pltpu.make_async_remote_copy(
            src_ref=block,
            dst_ref=block,
            send_sem=fwd_out.at[s, p],
            recv_sem=fwd_in.at[s, p],
            device_id={"dp": other},
            device_id_type=MESH,
        )

    def loads():
        copies = []
        for i in range(len(terms)):
            copies.append(pltpu.make_async_copy(weights[i].at[:, rows(i, me)], own_w[i], load_sem.at[i]))
        return copies

    count = range(len(pieces))
    for s in range(min(AHEAD, chips)):
        for p in count:
            fetch(s, p).start()

    barrier = pltpu.get_barrier_semaphore()
    for device in (other, onward, behind):
        pl.semaphore_signal(barrier, inc=1, device_id={"dp": device}, device_id_type=MESH)
    pl.semaphore_wait(barrier, 3)

    for s in range(min(AHEAD, chips)):
        for p in count:
            give(s, p).start()
    for copy in loads():
        copy.start()

    def total(s, p, tile):
        i, l = pieces[p]
        at = pl.ds(pl.multiple_of(tile * TILE, TILE), TILE)
        g = mine[i][s, l, at].astype(jnp.float32) + theirs[i][s, l, at].astype(jnp.float32)
        if s > 0:
            g = g + partial[i][s - 1, l, at].astype(jnp.float32)
        return at, g.astype(jnp.bfloat16)

    for s in range(chips - 1):
        for p in count:
            if s + AHEAD < chips:
                fetch(s + AHEAD, p).start()
                give(s + AHEAD, p).start()
            i, l = pieces[p]
            fetch(s, p).wait()
            give(s, p).wait_recv()
            if s > 0:
                send_sum(s - 1, p).wait_recv()

            @pl.loop(0, height[i] // TILE)
            def _(tile):
                at, g = total(s, p, tile)
                mine[i][s, l, at] = g

            send_sum(s, p).start()

    for copy in loads():
        copy.wait()
    last = chips - 1
    for p in count:
        i, l = pieces[p]
        fetch(last, p).wait()
        give(last, p).wait_recv()
        send_sum(last - 1, p).wait_recv()
        mine_rows = pl.multiple_of(me * height[i], TILE)

        @pl.loop(0, height[i] // TILE)
        def _(tile):
            at, g = total(last, p, tile)
            w, m, v = adamw(own_w[i][l, at].astype(jnp.float32), m_in[i][l, at], v_in[i][l, at], g.astype(jnp.float32))
            new[i][l, pl.ds(pl.multiple_of(mine_rows + tile * TILE, TILE), TILE)] = w
            m_out[i][l, at] = m
            v_out[i][l, at] = v

        send_new(0, p).start()
        forward(0, p).start()
    for s in range(1, chips):
        for p in count:
            send_new(s - 1, p).wait_recv()
            if s < last:
                send_new(s, p).start()
            forward(s, p).start()
    for s in range(chips):
        for p in count:
            forward(s, p).wait_recv()
            forward(s, p).wait_send()
            give(s, p).wait_send()
            if s < last:
                send_sum(s, p).wait_send()
                send_new(s, p).wait_send()


def solution(mesh):
    n = mesh.shape["dp"]
    chips = n // CORES

    def step(*arrays):
        terms, weights, m, v = (arrays[i : i + 3] for i in (0, 3, 6, 9))
        blocks = [one.shape for one in m]
        layers = blocks[0][0]
        count = len(m) * layers
        dma = pltpu.SemaphoreType.DMA

        def body(*refs):
            parts = [refs[i : i + 3] for i in range(0, 33, 3)]
            kernel(n, *parts, refs[33:])

        per_step = [pltpu.VMEM((chips, *shape), jnp.bfloat16) for shape in blocks]
        hops = [pltpu.VMEM((chips - 1, *shape), jnp.bfloat16) for shape in blocks]
        scratch = [*per_step, *per_step, *hops, *(pltpu.VMEM(shape, jnp.bfloat16) for shape in blocks)]
        semaphores = [dma((chips, count))] * 3 + [dma((len(m),))] + [dma((chips - 1, count))] * 4 + [dma((chips, count))] * 2
        anywhere, vmem = pl.BlockSpec(memory_space=pl.ANY), pl.BlockSpec(memory_space=pltpu.VMEM)
        return pl.pallas_call(
            body,
            out_shape=[jax.ShapeDtypeStruct(w.shape, w.dtype) for w in weights] + [jax.ShapeDtypeStruct(s, jnp.float32) for s in blocks] * 2,
            in_specs=[anywhere] * 6 + [vmem] * 6,
            out_specs=[vmem] * 9,
            scratch_shapes=[*scratch, *semaphores],
            compiler_params=pltpu.CompilerParams(collective_id=0, has_side_effects=True),
        )(*arrays)

    all_of, cut = P(None, None, None), P(None, "dp", None)
    return jax.shard_map(
        step,
        mesh=mesh,
        in_specs=(P(("rep", "dp"), None, None, None),) * 3 + (all_of,) * 3 + (cut,) * 6,
        out_specs=(P("rep", None, None),) * 3 + (P("rep", "dp", None),) * 6,
        check_vma=False,
    )
```

```python
import functools

import jax
import jax.numpy as jnp
from jax import lax
from jax.experimental import pallas as pl
from jax.experimental.pallas import tpu as pltpu
from jax.sharding import PartitionSpec as P

MESH = pl.DeviceIdType.MESH
CORES = 2
AHEAD = 2
TILE = 16
SCRATCH_BYTES = 43 << 20
WRITE_BYTES = 1 << 20


def adamw(w, m, v, g):
    m = 0.9 * m + 0.1 * g
    v = 0.95 * v + 0.05 * g * g
    step = m * lax.rsqrt(v + 1e-8) + 0.1 * w
    return (w - 0.02 * step).astype(jnp.bfloat16), m, v


def write_out(count, *refs):
    sources, places, sem = refs[:count], refs[count : 2 * count], refs[-1]
    copies = [pltpu.make_async_copy(a, b, sem.at[k]) for k, (a, b) in enumerate(zip(sources, places, strict=True))]
    for copy in copies:
        copy.start()
    for copy in copies:
        copy.wait()


def kernel(n, terms, weights, m_from, v_from, new, m_out, v_out, mine, theirs, partial, own_w, m_in, v_in, sems):
    (mine_sem, give_sem, take_sem, load_sem, sum_out, sum_in, ring_out, ring_in, fwd_out, fwd_in) = sems
    chips = n // CORES
    me = lax.axis_index("dp")
    chip, core = me // CORES, me % CORES
    way = 1 - CORES * core
    other = chip * CORES + (1 - core)

    def device_at(steps, which):
        return lax.rem(chip + way * steps + chips, chips) * CORES + which

    onward, behind = device_at(1, core), device_at(-1, core)
    layers = weights[0].shape[0]
    pieces = [(i, l) for i in range(len(terms)) for l in range(layers)]
    height = [ref.shape[2] for ref in mine]

    def rows(i, device):
        return pl.ds(pl.multiple_of(device * height[i], TILE), height[i])

    def fetch(s, p):
        i, l = pieces[p]
        return pltpu.make_async_copy(terms[i].at[0, l, rows(i, device_at(-1 - s, core))], mine[i].at[s, l], mine_sem.at[s, p])

    def give(s, p):
        i, l = pieces[p]
        return pltpu.make_async_remote_copy(
            src_ref=terms[i].at[0, l, rows(i, device_at(1 + s, 1 - core))],
            dst_ref=theirs[i].at[s, l],
            send_sem=give_sem.at[s, p],
            recv_sem=take_sem.at[s, p],
            device_id={"dp": other},
            device_id_type=MESH,
        )

    def send_sum(s, p):
        i, l = pieces[p]
        return pltpu.make_async_remote_copy(
            src_ref=mine[i].at[s, l],
            dst_ref=partial[i].at[s, l],
            send_sem=sum_out.at[s, p],
            recv_sem=sum_in.at[s, p],
            device_id={"dp": onward},
            device_id_type=MESH,
        )

    def send_new(s, p):
        i, l = pieces[p]
        block = new[i].at[l, rows(i, device_at(-s, core))]
        return pltpu.make_async_remote_copy(
            src_ref=block,
            dst_ref=block,
            send_sem=ring_out.at[s, p],
            recv_sem=ring_in.at[s, p],
            device_id={"dp": onward},
            device_id_type=MESH,
        )

    def forward(s, p):
        i, l = pieces[p]
        block = new[i].at[l, rows(i, device_at(-s, core))]
        return pltpu.make_async_remote_copy(
            src_ref=block,
            dst_ref=block,
            send_sem=fwd_out.at[s, p],
            recv_sem=fwd_in.at[s, p],
            device_id={"dp": other},
            device_id_type=MESH,
        )

    def loads():
        copies = []
        for i in range(len(terms)):
            copies.append(pltpu.make_async_copy(weights[i].at[:, rows(i, me)], own_w[i], load_sem.at[0, i]))
            copies.append(pltpu.make_async_copy(m_from[i], m_in[i], load_sem.at[1, i]))
            copies.append(pltpu.make_async_copy(v_from[i], v_in[i], load_sem.at[2, i]))
        return copies

    count = range(len(pieces))
    for s in range(min(AHEAD, chips)):
        for p in count:
            fetch(s, p).start()

    barrier = pltpu.get_barrier_semaphore()
    for device in (other, onward, behind):
        pl.semaphore_signal(barrier, inc=1, device_id={"dp": device}, device_id_type=MESH)
    pl.semaphore_wait(barrier, 3)

    for s in range(min(AHEAD, chips)):
        for p in count:
            give(s, p).start()
    for copy in loads():
        copy.start()

    def total(s, p, tile):
        i, l = pieces[p]
        at = pl.ds(pl.multiple_of(tile * TILE, TILE), TILE)
        g = mine[i][s, l, at].astype(jnp.float32) + theirs[i][s, l, at].astype(jnp.float32)
        if s > 0:
            g = g + partial[i][s - 1, l, at].astype(jnp.float32)
        return at, g.astype(jnp.bfloat16)

    for s in range(chips - 1):
        for p in count:
            if s + AHEAD < chips:
                fetch(s + AHEAD, p).start()
                give(s + AHEAD, p).start()
            i, l = pieces[p]
            fetch(s, p).wait()
            give(s, p).wait_recv()
            if s > 0:
                send_sum(s - 1, p).wait_recv()

            @pl.loop(0, height[i] // TILE)
            def _(tile):
                at, g = total(s, p, tile)
                mine[i][s, l, at] = g

            send_sum(s, p).start()

    for copy in loads():
        copy.wait()
    last = chips - 1
    for p in count:
        i, l = pieces[p]
        fetch(last, p).wait()
        give(last, p).wait_recv()
        send_sum(last - 1, p).wait_recv()
        mine_rows = pl.multiple_of(me * height[i], TILE)

        @pl.loop(0, height[i] // TILE)
        def _(tile):
            at, g = total(last, p, tile)
            w, m, v = adamw(own_w[i][l, at].astype(jnp.float32), m_in[i][l, at], v_in[i][l, at], g.astype(jnp.float32))
            new[i][l, pl.ds(pl.multiple_of(mine_rows + tile * TILE, TILE), TILE)] = w
            m_out[i][l, at] = m
            v_out[i][l, at] = v

        send_new(0, p).start()
        forward(0, p).start()
    for s in range(1, chips):
        for p in count:
            send_new(s - 1, p).wait_recv()
            if s < last:
                send_new(s, p).start()
            forward(s, p).start()
    for s in range(chips):
        for p in count:
            forward(s, p).wait_recv()
            forward(s, p).wait_send()
            give(s, p).wait_send()
            if s < last:
                send_sum(s, p).wait_send()
                send_new(s, p).wait_send()


def solution(mesh):
    n = mesh.shape["dp"]
    chips = n // CORES

    def step(*arrays):
        terms, weights, m, v = (arrays[i : i + 3] for i in (0, 3, 6, 9))
        blocks = [one.shape for one in m]
        layers = blocks[0][0]
        count = len(m) * layers
        dma = pltpu.SemaphoreType.DMA

        def body(*refs):
            parts = [refs[i : i + 3] for i in range(0, 39, 3)]
            kernel(n, *parts, refs[39:])

        per_step = [pltpu.VMEM((chips, *shape), jnp.bfloat16) for shape in blocks]
        hops = [pltpu.VMEM((chips - 1, *shape), jnp.bfloat16) for shape in blocks]
        moments = [pltpu.VMEM(shape, jnp.float32) for shape in blocks]
        scratch = [*per_step, *per_step, *hops, *(pltpu.VMEM(shape, jnp.bfloat16) for shape in blocks), *moments, *moments]
        semaphores = [dma((chips, count))] * 3 + [dma((3, len(m)))] + [dma((chips - 1, count))] * 4 + [dma((chips, count))] * 2
        hbm, vmem = pl.BlockSpec(memory_space=pltpu.HBM), pl.BlockSpec(memory_space=pltpu.VMEM)
        shapes = [jax.ShapeDtypeStruct(w.shape, w.dtype) for w in weights] + [jax.ShapeDtypeStruct(s, jnp.float32) for s in blocks] * 2
        inside = pl.pallas_call(
            body,
            out_shape=[pltpu.VMEM(one.shape, one.dtype) for one in shapes],
            in_specs=[hbm] * len(arrays),
            out_specs=[vmem] * len(shapes),
            scratch_shapes=[*scratch, *semaphores],
            compiler_params=pltpu.CompilerParams(collective_id=0, has_side_effects=True, vmem_limit_bytes=SCRATCH_BYTES),
        )(*arrays)
        return pl.pallas_call(
            functools.partial(write_out, len(shapes)),
            out_shape=shapes,
            in_specs=[vmem] * len(shapes),
            out_specs=[hbm] * len(shapes),
            scratch_shapes=[dma((len(shapes),))],
            compiler_params=pltpu.CompilerParams(vmem_limit_bytes=WRITE_BYTES),
        )(*inside)

    all_of, cut = P(None, None, None), P(None, "dp", None)
    return jax.shard_map(
        step,
        mesh=mesh,
        in_specs=(P(("rep", "dp"), None, None, None),) * 3 + (all_of,) * 3 + (cut,) * 6,
        out_specs=(P("rep", None, None),) * 3 + (P("rep", "dp", None),) * 6,
        check_vma=False,
    )
```

```python
import functools

import jax
import jax.numpy as jnp
from jax import lax
from jax.experimental import pallas as pl
from jax.experimental.pallas import tpu as pltpu
from jax.sharding import PartitionSpec as P

MESH = pl.DeviceIdType.MESH
CORES = 2
AHEAD = 2
TILE = 16
SCRATCH_BYTES = 43 << 20
WRITE_BYTES = 1 << 20


def adamw(w, m, v, g):
    m = 0.9 * m + 0.1 * g
    v = 0.95 * v + 0.05 * g * g
    step = m * lax.rsqrt(v + 1e-8) + 0.1 * w
    return (w - 0.02 * step).astype(jnp.bfloat16), m, v


def write_out(count, *refs):
    sources, places, sem = refs[:count], refs[count : 2 * count], refs[-1]
    copies = [pltpu.make_async_copy(a, b, sem.at[k]) for k, (a, b) in enumerate(zip(sources, places, strict=True))]
    for copy in copies:
        copy.start()
    for copy in copies:
        copy.wait()


def cut(blocks, first, last):
    coarse = [(i, (0, shape[0]), (0, shape[1])) for i, shape in enumerate(blocks)]
    single = [(i, (l, l + 1), (0, shape[1])) for i, shape in enumerate(blocks) for l in range(shape[0])]

    def split(piece, parts):
        i, layers, (low, high) = piece
        tiles, at, out = (high - low) // TILE, low, []
        for k in range(parts):
            size = (tiles // (parts - k)) * TILE
            tiles -= size // TILE
            out.append((i, layers, (at, at + size)))
            at += size
        return out

    fine_first = [*split(single[0], first), *single[1:]]
    fine_last = [*single[:-1], *split(single[-1], last)]
    return coarse, fine_first, fine_last


def kernel(n, cuts, terms, weights, m_from, v_from, new, m_out, v_out, mine, theirs, partial, own_w, m_in, v_in, stage, sems):
    (mine_sem, stage_sem, give_sem, take_sem, load_sem, sum_out, sum_in, ring_out, ring_in, fwd_out, fwd_in) = sems
    coarse, fine_first, fine_last = cuts
    chips = n // CORES
    last = chips - 1
    me = lax.axis_index("dp")
    chip, core = me // CORES, me % CORES
    way = 1 - CORES * core
    other = chip * CORES + (1 - core)

    def device_at(steps, which):
        return lax.rem(chip + way * steps + chips, chips) * CORES + which

    onward, behind = device_at(1, core), device_at(-1, core)
    height = [ref.shape[2] for ref in mine]

    def remote(source, place, send_sem, recv_sem, device):
        return pltpu.make_async_remote_copy(
            src_ref=source, dst_ref=place, send_sem=send_sem, recv_sem=recv_sem, device_id={"dp": device}, device_id_type=MESH
        )

    def span(piece):
        _, (l0, l1), (r0, r1) = piece
        return pl.ds(l0, l1 - l0), pl.ds(r0, r1 - r0)

    def rows(piece, device):
        i, _, (r0, r1) = piece
        return pl.ds(pl.multiple_of(device * height[i] + r0, TILE), r1 - r0)

    def cut_of_sum(s):
        return fine_first if s == 0 else coarse

    def cut_of_new(s):
        return fine_last if s >= last - 1 else coarse

    def fetch(s, p):
        piece = cut_of_sum(s)[p]
        layers, within = span(piece)
        source = terms[piece[0]].at[0, layers, rows(piece, device_at(-1 - s, core))]
        return pltpu.make_async_copy(source, mine[piece[0]].at[s, layers, within], mine_sem.at[s, p])

    def set_stage(p):
        piece = cut_of_sum(0)[p]
        layers, within = span(piece)
        source = terms[piece[0]].at[0, layers, rows(piece, device_at(1, 1 - core))]
        return pltpu.make_async_copy(source, stage[piece[0]].at[layers, within], stage_sem.at[p])

    def give(s, p):
        piece = cut_of_sum(s)[p]
        layers, within = span(piece)
        if s == 0:
            source = stage[piece[0]].at[layers, within]
        else:
            source = terms[piece[0]].at[0, layers, rows(piece, device_at(1 + s, 1 - core))]
        return remote(source, theirs[piece[0]].at[s, layers, within], give_sem.at[s, p], take_sem.at[s, p], other)

    def send_sum(s, p):
        piece = cut_of_sum(s)[p]
        layers, within = span(piece)
        i = piece[0]
        return remote(mine[i].at[s, layers, within], partial[i].at[s, layers, within], sum_out.at[s, p], sum_in.at[s, p], onward)

    def new_block(s, piece):
        return new[piece[0]].at[span(piece)[0], rows(piece, device_at(-s, core))]

    def send_new(s, p):
        block = new_block(s, cut_of_new(s)[p])
        return remote(block, block, ring_out.at[s, p], ring_in.at[s, p], onward)

    def forward(s, p):
        block = new_block(s, cut_of_new(max(s - 1, 0))[p])
        return remote(block, block, fwd_out.at[s, p], fwd_in.at[s, p], other)

    def load(i):
        return [
            pltpu.make_async_copy(weights[i].at[:, pl.ds(pl.multiple_of(me * height[i], TILE), height[i])], own_w[i], load_sem.at[0, i]),
            pltpu.make_async_copy(m_from[i], m_in[i], load_sem.at[1, i]),
            pltpu.make_async_copy(v_from[i], v_in[i], load_sem.at[2, i]),
        ]

    def every(s):
        return range(len(cut_of_sum(s)))

    barrier = pltpu.get_barrier_semaphore()
    for device in (other, onward, behind):
        pl.semaphore_signal(barrier, inc=1, device_id={"dp": device}, device_id_type=MESH)
    for p in every(0):
        set_stage(p).start()
        fetch(0, p).start()
    set_stage(0).wait()
    pl.semaphore_wait(barrier, 3)
    for p in every(0):
        if p:
            set_stage(p).wait()
        give(0, p).start()
    for s in range(1, AHEAD):
        for p in every(s):
            fetch(s, p).start()
            give(s, p).start()

    def over_tiles(piece, do):
        i, (l0, l1), (r0, r1) = piece
        for l in range(l0, l1):

            @pl.loop(r0 // TILE, r1 // TILE)
            def _(tile):
                do(i, l, tile, pl.ds(pl.multiple_of(tile * TILE, TILE), TILE))

    def total(s, i, l, at):
        g = mine[i][s, l, at].astype(jnp.float32) + theirs[i][s, l, at].astype(jnp.float32)
        if s > 0:
            g = g + partial[i][s - 1, l, at].astype(jnp.float32)
        return g.astype(jnp.bfloat16)

    def wait_parts(s, p):
        for q, piece in enumerate(cut_of_sum(s - 1)):
            if piece[0] == cut_of_sum(s)[p][0]:
                send_sum(s - 1, q).wait_recv()

    for s in range(chips - 1):
        for p in every(s):
            fetch(s, p).wait()
            give(s, p).wait_recv()
            if s > 0:
                wait_parts(s, p)

            def add(i, l, tile, at):
                mine[i][s, l, at] = total(s, i, l, at)

            over_tiles(cut_of_sum(s)[p], add)
            send_sum(s, p).start()
        if s + AHEAD < chips:
            for p in every(s + AHEAD):
                fetch(s + AHEAD, p).start()
                give(s + AHEAD, p).start()
        if s == 0:
            for i in range(len(weights)):
                for copy in load(i):
                    copy.start()

    for p, piece in enumerate(coarse):
        i = piece[0]
        for copy in load(i):
            copy.wait()
        fetch(last, p).wait()
        give(last, p).wait_recv()
        wait_parts(last, p)
        start = pl.multiple_of(me * height[i], TILE)

        def take_step(i, l, tile, at):
            g = total(last, i, l, at).astype(jnp.float32)
            w, m, v = adamw(own_w[i][l, at].astype(jnp.float32), m_in[i][l, at], v_in[i][l, at], g)
            new[i][l, pl.ds(pl.multiple_of(start + tile * TILE, TILE), TILE)] = w
            m_out[i][l, at] = m
            v_out[i][l, at] = v

        over_tiles(piece, take_step)
        send_new(0, p).start()
        forward(0, p).start()
    for s in range(1, chips):
        came = cut_of_new(s - 1)
        if s < last and cut_of_new(s) is not came:
            for p, piece in enumerate(came):
                send_new(s - 1, p).wait_recv()
                for q, finer in enumerate(cut_of_new(s)):
                    if finer[0] == piece[0]:
                        send_new(s, q).start()
                forward(s, p).start()
        else:
            for p in range(len(came)):
                send_new(s - 1, p).wait_recv()
                if s < last:
                    send_new(s, p).start()
                forward(s, p).start()
    for s in range(chips):
        for p in every(s):
            give(s, p).wait_send()
            if s < last:
                send_sum(s, p).wait_send()
        for p in range(len(cut_of_new(s))):
            if s < last:
                send_new(s, p).wait_send()
        for p in range(len(cut_of_new(max(s - 1, 0)))):
            forward(s, p).wait_send()
            forward(s, p).wait_recv()


def solution(mesh):
    n = mesh.shape["dp"]
    chips = n // CORES

    def step(*arrays):
        terms, weights, m, v = (arrays[i : i + 3] for i in (0, 3, 6, 9))
        blocks = [one.shape for one in m]
        cuts = cut(blocks, 3, 3)
        count = max(len(one) for one in cuts)
        dma = pltpu.SemaphoreType.DMA

        def body(*refs):
            parts = [refs[i : i + 3] for i in range(0, 42, 3)]
            kernel(n, cuts, *parts, refs[42:])

        per_step = [pltpu.VMEM((chips, *shape), jnp.bfloat16) for shape in blocks]
        hops = [pltpu.VMEM((chips - 1, *shape), jnp.bfloat16) for shape in blocks]
        block = [pltpu.VMEM(shape, jnp.bfloat16) for shape in blocks]
        moments = [pltpu.VMEM(shape, jnp.float32) for shape in blocks]
        scratch = [*per_step, *per_step, *hops, *block, *moments, *moments, *block]
        semaphores = [
            dma((chips, count)),
            dma((count,)),
            *[dma((chips, count))] * 2,
            dma((3, len(m))),
            *[dma((chips - 1, count))] * 4,
            *[dma((chips, count))] * 2,
        ]
        hbm, vmem = pl.BlockSpec(memory_space=pltpu.HBM), pl.BlockSpec(memory_space=pltpu.VMEM)
        shapes = [jax.ShapeDtypeStruct(w.shape, w.dtype) for w in weights] + [jax.ShapeDtypeStruct(s, jnp.float32) for s in blocks] * 2
        inside = pl.pallas_call(
            body,
            out_shape=[pltpu.VMEM(one.shape, one.dtype) for one in shapes],
            in_specs=[hbm] * len(arrays),
            out_specs=[vmem] * len(shapes),
            scratch_shapes=[*scratch, *semaphores],
            compiler_params=pltpu.CompilerParams(collective_id=0, has_side_effects=True, vmem_limit_bytes=SCRATCH_BYTES),
        )(*arrays)
        return pl.pallas_call(
            functools.partial(write_out, len(shapes)),
            out_shape=shapes,
            in_specs=[vmem] * len(shapes),
            out_specs=[hbm] * len(shapes),
            scratch_shapes=[dma((len(shapes),))],
            compiler_params=pltpu.CompilerParams(vmem_limit_bytes=WRITE_BYTES),
        )(*inside)

    all_of, shared = P(None, None, None), P(None, "dp", None)
    return jax.shard_map(
        step,
        mesh=mesh,
        in_specs=(P(("rep", "dp"), None, None, None),) * 3 + (all_of,) * 3 + (shared,) * 6,
        out_specs=(P("rep", None, None),) * 3 + (P("rep", "dp", None),) * 6,
        check_vma=False,
    )
```

```python
import functools

import jax
import jax.numpy as jnp
from jax import lax
from jax.experimental import pallas as pl
from jax.experimental.pallas import tpu as pltpu
from jax.sharding import PartitionSpec as P

MESH = pl.DeviceIdType.MESH
CORES = 2
AHEAD = 2
FIRST = 1
LAST = 1
COARSE = True
STAGE = False
TILE = 16
SCRATCH_BYTES = 43 << 20
WRITE_BYTES = 1 << 20


def adamw(w, m, v, g):
    m = 0.9 * m + 0.1 * g
    v = 0.95 * v + 0.05 * g * g
    step = m * lax.rsqrt(v + 1e-8) + 0.1 * w
    return (w - 0.02 * step).astype(jnp.bfloat16), m, v


def write_out(count, *refs):
    sources, places, sem = refs[:count], refs[count : 2 * count], refs[-1]
    copies = [pltpu.make_async_copy(a, b, sem.at[k]) for k, (a, b) in enumerate(zip(sources, places, strict=True))]
    for copy in copies:
        copy.start()
    for copy in copies:
        copy.wait()


def cut(blocks, first, last):
    coarse = [(i, (0, shape[0]), (0, shape[1])) for i, shape in enumerate(blocks)]
    single = [(i, (l, l + 1), (0, shape[1])) for i, shape in enumerate(blocks) for l in range(shape[0])]

    def split(piece, parts):
        i, layers, (low, high) = piece
        tiles, at, out = (high - low) // TILE, low, []
        for k in range(parts):
            size = (tiles // (parts - k)) * TILE
            tiles -= size // TILE
            out.append((i, layers, (at, at + size)))
            at += size
        return out

    fine_first = [*split(single[0], first), *single[1:]]
    fine_last = [*single[:-1], *split(single[-1], last)]
    return coarse if COARSE else single, fine_first, fine_last


def inside(small, large):
    (i, (l0, l1), (r0, r1)), (j, (k0, k1), (q0, q1)) = small, large
    return i == j and k0 <= l0 and l1 <= k1 and q0 <= r0 and r1 <= q1


def kernel(n, cuts, terms, weights, m_from, v_from, new, m_out, v_out, mine, theirs, partial, own_w, m_in, v_in, stage, sems):
    (mine_sem, stage_sem, give_sem, take_sem, load_sem, sum_out, sum_in, ring_out, ring_in, fwd_out, fwd_in) = sems
    coarse, fine_first, fine_last = cuts
    chips = n // CORES
    last = chips - 1
    me = lax.axis_index("dp")
    chip, core = me // CORES, me % CORES
    way = 1 - CORES * core
    other = chip * CORES + (1 - core)

    def device_at(steps, which):
        return lax.rem(chip + way * steps + chips, chips) * CORES + which

    onward, behind = device_at(1, core), device_at(-1, core)
    height = [ref.shape[2] for ref in mine]

    def remote(source, place, send_sem, recv_sem, device):
        return pltpu.make_async_remote_copy(
            src_ref=source, dst_ref=place, send_sem=send_sem, recv_sem=recv_sem, device_id={"dp": device}, device_id_type=MESH
        )

    def span(piece):
        _, (l0, l1), (r0, r1) = piece
        return pl.ds(l0, l1 - l0), pl.ds(r0, r1 - r0)

    def rows(piece, device):
        i, _, (r0, r1) = piece
        return pl.ds(pl.multiple_of(device * height[i] + r0, TILE), r1 - r0)

    def cut_of_sum(s):
        return fine_first if s == 0 else coarse

    def cut_of_new(s):
        return fine_last if s >= last - 1 else coarse

    def fetch(s, p):
        piece = cut_of_sum(s)[p]
        layers, within = span(piece)
        source = terms[piece[0]].at[0, layers, rows(piece, device_at(-1 - s, core))]
        return pltpu.make_async_copy(source, mine[piece[0]].at[s, layers, within], mine_sem.at[s, p])

    def set_stage(p):
        piece = cut_of_sum(0)[p]
        layers, within = span(piece)
        source = terms[piece[0]].at[0, layers, rows(piece, device_at(1, 1 - core))]
        return pltpu.make_async_copy(source, stage[piece[0]].at[layers, within], stage_sem.at[p])

    def give(s, p):
        piece = cut_of_sum(s)[p]
        layers, within = span(piece)
        if s == 0 and STAGE:
            source = stage[piece[0]].at[layers, within]
        else:
            source = terms[piece[0]].at[0, layers, rows(piece, device_at(1 + s, 1 - core))]
        return remote(source, theirs[piece[0]].at[s, layers, within], give_sem.at[piece[0]], take_sem.at[s, p], other)

    def send_sum(s, p):
        piece = cut_of_sum(s)[p]
        layers, within = span(piece)
        i = piece[0]
        return remote(mine[i].at[s, layers, within], partial[i].at[s, layers, within], sum_out.at[i], sum_in.at[s, p], onward)

    def new_block(s, piece):
        return new[piece[0]].at[span(piece)[0], rows(piece, device_at(-s, core))]

    def send_new(s, p):
        piece = cut_of_new(s)[p]
        block = new_block(s, piece)
        return remote(block, block, ring_out.at[piece[0]], ring_in.at[s, p], onward)

    def forward(s, p):
        piece = cut_of_new(max(s - 1, 0))[p]
        block = new_block(s, piece)
        return remote(block, block, fwd_out.at[piece[0]], fwd_in.at[piece[0]], other)

    def load(i):
        return [
            pltpu.make_async_copy(weights[i].at[:, pl.ds(pl.multiple_of(me * height[i], TILE), height[i])], own_w[i], load_sem.at[0, i]),
            pltpu.make_async_copy(m_from[i], m_in[i], load_sem.at[1, i]),
            pltpu.make_async_copy(v_from[i], v_in[i], load_sem.at[2, i]),
        ]

    def every(s):
        return range(len(cut_of_sum(s)))

    barrier = pltpu.get_barrier_semaphore()
    for device in (other, onward, behind):
        pl.semaphore_signal(barrier, inc=1, device_id={"dp": device}, device_id_type=MESH)
    for p in every(0):
        if STAGE:
            set_stage(p).start()
        fetch(0, p).start()
    if STAGE:
        set_stage(0).wait()
    pl.semaphore_wait(barrier, 3)
    for p in every(0):
        if p and STAGE:
            set_stage(p).wait()
        give(0, p).start()
    for s in range(1, AHEAD):
        for p in every(s):
            fetch(s, p).start()
            give(s, p).start()

    def over_tiles(piece, do):
        i, (l0, l1), (r0, r1) = piece
        for l in range(l0, l1):

            @pl.loop(r0 // TILE, r1 // TILE)
            def _(tile):
                do(i, l, tile, pl.ds(pl.multiple_of(tile * TILE, TILE), TILE))

    def total(s, i, l, at):
        g = mine[i][s, l, at].astype(jnp.float32) + theirs[i][s, l, at].astype(jnp.float32)
        if s > 0:
            g = g + partial[i][s - 1, l, at].astype(jnp.float32)
        return g.astype(jnp.bfloat16)

    def wait_parts(s, p):
        for q, piece in enumerate(cut_of_sum(s - 1)):
            if inside(piece, cut_of_sum(s)[p]):
                send_sum(s - 1, q).wait_recv()

    for s in range(chips - 1):
        for p in every(s):
            fetch(s, p).wait()
            give(s, p).wait_recv()
            if s > 0:
                wait_parts(s, p)

            def add(i, l, tile, at):
                mine[i][s, l, at] = total(s, i, l, at)

            over_tiles(cut_of_sum(s)[p], add)
            send_sum(s, p).start()
        if s + AHEAD < chips:
            for p in every(s + AHEAD):
                fetch(s + AHEAD, p).start()
                give(s + AHEAD, p).start()
        if s == 0:
            for i in range(len(weights)):
                for copy in load(i):
                    copy.start()

    for p, piece in enumerate(coarse):
        i = piece[0]
        if p == 0 or coarse[p - 1][0] != i:
            for copy in load(i):
                copy.wait()
        fetch(last, p).wait()
        give(last, p).wait_recv()
        wait_parts(last, p)
        start = pl.multiple_of(me * height[i], TILE)

        def take_step(i, l, tile, at):
            g = total(last, i, l, at).astype(jnp.float32)
            w, m, v = adamw(own_w[i][l, at].astype(jnp.float32), m_in[i][l, at], v_in[i][l, at], g)
            new[i][l, pl.ds(pl.multiple_of(start + tile * TILE, TILE), TILE)] = w
            m_out[i][l, at] = m
            v_out[i][l, at] = v

        over_tiles(piece, take_step)
        send_new(0, p).start()
        forward(0, p).start()
    for s in range(1, chips):
        came = cut_of_new(s - 1)
        if s < last and cut_of_new(s) is not came:
            for p, piece in enumerate(came):
                send_new(s - 1, p).wait_recv()
                for q, finer in enumerate(cut_of_new(s)):
                    if inside(finer, piece):
                        send_new(s, q).start()
                forward(s, p).start()
        else:
            for p in range(len(came)):
                send_new(s - 1, p).wait_recv()
                if s < last:
                    send_new(s, p).start()
                forward(s, p).start()
    for i in range(len(terms)):
        some = new[i].at[:, pl.ds(0, last * height[i])]
        remote(theirs[i], theirs[i], give_sem.at[i], fwd_in.at[i], other).wait_send()
        remote(partial[i], partial[i], sum_out.at[i], fwd_in.at[i], onward).wait_send()
        remote(some, some, ring_out.at[i], fwd_in.at[i], onward).wait_send()
        whole = remote(theirs[i], theirs[i], fwd_out.at[i], fwd_in.at[i], other)
        whole.wait_send()
        whole.wait_recv()


def solution(mesh):
    n = mesh.shape["dp"]
    chips = n // CORES

    def step(*arrays):
        terms, weights, m, v = (arrays[i : i + 3] for i in (0, 3, 6, 9))
        blocks = [one.shape for one in m]
        cuts = cut(blocks, FIRST, LAST)
        count = max(len(one) for one in cuts)
        dma = pltpu.SemaphoreType.DMA

        def body(*refs):
            parts = [refs[i : i + 3] for i in range(0, 42, 3)]
            kernel(n, cuts, *parts, refs[42:])

        per_step = [pltpu.VMEM((chips, *shape), jnp.bfloat16) for shape in blocks]
        hops = [pltpu.VMEM((chips - 1, *shape), jnp.bfloat16) for shape in blocks]
        block = [pltpu.VMEM(shape, jnp.bfloat16) for shape in blocks]
        moments = [pltpu.VMEM(shape, jnp.float32) for shape in blocks]
        scratch = [*per_step, *per_step, *hops, *block, *moments, *moments, *block]
        each, hop = dma((chips, count)), dma((chips - 1, count))
        one = dma((len(m),))
        semaphores = [each, dma((count,)), one, each, dma((3, len(m))), one, hop, one, hop, one, one]
        hbm, vmem = pl.BlockSpec(memory_space=pltpu.HBM), pl.BlockSpec(memory_space=pltpu.VMEM)
        shapes = [jax.ShapeDtypeStruct(w.shape, w.dtype) for w in weights] + [jax.ShapeDtypeStruct(b, jnp.float32) for b in blocks] * 2
        inside = pl.pallas_call(
            body,
            out_shape=[pltpu.VMEM(one.shape, one.dtype) for one in shapes],
            in_specs=[hbm] * len(arrays),
            out_specs=[vmem] * len(shapes),
            scratch_shapes=[*scratch, *semaphores],
            compiler_params=pltpu.CompilerParams(collective_id=0, has_side_effects=True, vmem_limit_bytes=SCRATCH_BYTES),
        )(*arrays)
        return pl.pallas_call(
            functools.partial(write_out, len(shapes)),
            out_shape=shapes,
            in_specs=[vmem] * len(shapes),
            out_specs=[hbm] * len(shapes),
            scratch_shapes=[dma((len(shapes),))],
            compiler_params=pltpu.CompilerParams(vmem_limit_bytes=WRITE_BYTES),
        )(*inside)

    all_of, shared = P(None, None, None), P(None, "dp", None)
    return jax.shard_map(
        step,
        mesh=mesh,
        in_specs=(P(("rep", "dp"), None, None, None),) * 3 + (all_of,) * 3 + (shared,) * 6,
        out_specs=(P("rep", None, None),) * 3 + (P("rep", "dp", None),) * 6,
        check_vma=False,
    )
```

```python
import functools

import jax
import jax.numpy as jnp
from jax import lax
from jax.experimental import pallas as pl
from jax.experimental.pallas import tpu as pltpu
from jax.sharding import PartitionSpec as P

MESH = pl.DeviceIdType.MESH
CORES = 2
AHEAD = 2
FIRST = (1,)
LAST = (1, 2)
TILE = 16
SCRATCH_BYTES = 43 << 20
WRITE_BYTES = 1 << 20


def adamw(w, m, v, g):
    m = 0.9 * m + 0.1 * g
    v = 0.95 * v + 0.05 * g * g
    step = m * lax.rsqrt(v + 1e-8) + 0.1 * w
    return (w - 0.02 * step).astype(jnp.bfloat16), m, v


def write_out(count, *refs):
    sources, places, sem = refs[:count], refs[count : 2 * count], refs[-1]
    copies = [pltpu.make_async_copy(a, b, sem.at[k]) for k, (a, b) in enumerate(zip(sources, places, strict=True))]
    for copy in copies:
        copy.start()
    for copy in copies:
        copy.wait()


def cut(shape, sizes, backwards):
    layers, height = shape[:2]
    ends, at = [], 0
    for size in sizes:
        ends.append((at, at + size * TILE))
        at += size * TILE
    ends.append((at, height))
    if backwards:
        ends = [(height - high, height - low) for low, high in reversed(ends)]
        return [((0, layers - 1), (0, height)), *[((layers - 1, layers), one) for one in ends]]
    return [*[((0, 1), one) for one in ends], ((1, layers), (0, height))]


def kernel(n, terms, weights, m_from, v_from, new, m_out, v_out, mine, theirs, partial, own_w, m_in, v_in, sems):
    mine_sem, take_sem, first_sem, hop_sem, end_sem, load_sem, chip_out, ring_out, fwd_in = sems
    chips = n // CORES
    last = chips - 1
    me = lax.axis_index("dp")
    chip, core = me // CORES, me % CORES
    way = 1 - CORES * core
    other = chip * CORES + (1 - core)
    shapes = [ref.shape[1:] for ref in mine]
    height = [shape[1] for shape in shapes]
    every = range(len(terms))
    whole = [[((0, shape[0]), (0, shape[1]))] for shape in shapes]
    first, final = [*whole], [*whole]
    first[0] = cut(shapes[0], FIRST, False)
    final[-1] = cut(shapes[-1], LAST, True)

    def device_at(steps, which):
        return lax.rem(chip + way * steps + chips, chips) * CORES + which

    onward = device_at(1, core)

    def remote(source, place, send_sem, recv_sem, device):
        return pltpu.make_async_remote_copy(
            src_ref=source, dst_ref=place, send_sem=send_sem, recv_sem=recv_sem, device_id={"dp": device}, device_id_type=MESH
        )

    def rows(i, device, part=None):
        low, high = part or (0, height[i])
        return pl.ds(pl.multiple_of(device * height[i] + low, TILE), high - low)

    def span(low, high):
        return pl.ds(low, high - low)

    def fetch(s, i):
        source = terms[i].at[0, :, rows(i, device_at(-1 - s, core))]
        return pltpu.make_async_copy(source, mine[i].at[s], mine_sem.at[s % AHEAD, i])

    def parts_of_sum(s, i):
        return first[i] if s == 0 else whole[i]

    def parts_of_new(s, i):
        return final[i] if s == last - 1 else whole[i]

    def give(s, i, k):
        layers, part = parts_of_sum(s, i)[k]
        sem = first_sem.at[k] if len(parts_of_sum(s, i)) > 1 else take_sem.at[s % (2 * AHEAD), i]
        source = terms[i].at[0, span(*layers), rows(i, device_at(1 + s, 1 - core), part)]
        return remote(source, theirs[i].at[s, span(*layers), span(*part)], chip_out.at[i], sem, other)

    def give_all(s):
        for i in every:
            for k in range(len(parts_of_sum(s, i))):
                give(s, i, k).start()

    def send_sum(s, i, k=None):
        layers, part = whole[i][0] if k is None else parts_of_sum(s, i)[k]
        source, place = (ref[i].at[s, span(*layers), span(*part)] for ref in (mine, partial))
        return remote(source, place, ring_out.at[i], hop_sem.at[s % chips, i], onward)

    def new_block(s, i, k, came):
        layers, part = parts_of_new(s - 1 if came else s, i)[k]
        return new[i].at[span(*layers), rows(i, device_at(-s, core), part)]

    def send_new(s, i, k):
        block = new_block(s, i, k, False)
        sem = end_sem.at[k] if len(parts_of_new(s, i)) > 1 else hop_sem.at[(last + s) % chips, i]
        return remote(block, block, ring_out.at[i], sem, onward)

    def forward(s, i, k):
        block = new_block(s, i, k, s > 0)
        return remote(block, block, chip_out.at[i], fwd_in.at[i], other)

    def load(i):
        return [
            pltpu.make_async_copy(weights[i].at[:, rows(i, me)], own_w[i], load_sem.at[i]),
            pltpu.make_async_copy(m_from[i], m_in[i], load_sem.at[i]),
            pltpu.make_async_copy(v_from[i], v_in[i], load_sem.at[i]),
        ]

    barrier = pltpu.get_barrier_semaphore()
    for device in (other, onward, device_at(-1, core)):
        pl.semaphore_signal(barrier, inc=1, device_id={"dp": device}, device_id_type=MESH)
    for i in every:
        fetch(0, i).start()
    pl.semaphore_wait(barrier, 3)
    give_all(0)
    for s in range(1, AHEAD):
        for i in every:
            fetch(s, i).start()
        give_all(s)

    def over_tiles(i, layers, part, do):
        for l in range(*layers):

            @pl.loop(part[0] // TILE, part[1] // TILE)
            def _(tile):
                do(i, l, tile, pl.ds(pl.multiple_of(tile * TILE, TILE), TILE))

    def total(s, i, l, at):
        g = mine[i][s, l, at].astype(jnp.float32) + theirs[i][s, l, at].astype(jnp.float32)
        if s > 0:
            g = g + partial[i][s - 1, l, at].astype(jnp.float32)
        return g.astype(jnp.bfloat16)

    for s in range(last):
        for i in every:
            fetch(s, i).wait()
            if s > 0:
                send_sum(s - 1, i).wait_recv()
            for k, (layers, part) in enumerate(parts_of_sum(s, i)):
                give(s, i, k).wait_recv()

                def add(i, l, tile, at):
                    mine[i][s, l, at] = total(s, i, l, at)

                over_tiles(i, layers, part, add)
                send_sum(s, i, k).start()
        if s + AHEAD < chips:
            for i in every:
                fetch(s + AHEAD, i).start()
            give_all(s + AHEAD)
        if s == 0:
            for i in every:
                for copy in load(i):
                    copy.start()

    for i in every:
        five = pl.ds(0, 5 * height[i])
        pltpu.make_async_copy(terms[i].at[0, :, five], new[i].at[:, five], load_sem.at[i]).wait()
        fetch(last, i).wait()
        give(last, i, 0).wait_recv()
        send_sum(last - 1, i).wait_recv()
        start = pl.multiple_of(me * height[i], TILE)

        def take_step(i, l, tile, at):
            g = total(last, i, l, at).astype(jnp.float32)
            w, m, v = adamw(own_w[i][l, at].astype(jnp.float32), m_in[i][l, at], v_in[i][l, at], g)
            new[i][l, pl.ds(pl.multiple_of(start + tile * TILE, TILE), TILE)] = w
            m_out[i][l, at] = m
            v_out[i][l, at] = v

        over_tiles(i, *whole[i][0], take_step)
        send_new(0, i, 0).start()
        forward(0, i, 0).start()
    for s in range(1, chips):
        for i in every:
            came = parts_of_new(s - 1, i)
            for k in range(len(came)):
                send_new(s - 1, i, k).wait_recv()
                if s < last and k == 0:
                    for q in range(len(parts_of_new(s, i))):
                        send_new(s, i, q).start()
                forward(s, i, k).start()
    for i in every:
        ring = new[i].at[:, pl.ds(0, 2 * last * height[i])]
        remote(ring, ring, ring_out.at[i], fwd_in.at[i], onward).wait_send()
        remote(new[i], new[i], chip_out.at[i], fwd_in.at[i], other).wait_send()
        half = new[i].at[:, pl.ds(0, chips * height[i])]
        remote(half, half, chip_out.at[i], fwd_in.at[i], other).wait_recv()


def solution(mesh):
    n = mesh.shape["dp"]
    chips = n // CORES

    def step(*arrays):
        terms, weights, m, v = (arrays[i : i + 3] for i in (0, 3, 6, 9))
        blocks = [one.shape for one in m]
        count = len(blocks)
        dma = pltpu.SemaphoreType.DMA

        def body(*refs):
            parts = [refs[i : i + 3] for i in range(0, 39, 3)]
            kernel(n, *parts, refs[39:])

        per_step = [pltpu.VMEM((chips, *shape), jnp.bfloat16) for shape in blocks]
        hops = [pltpu.VMEM((chips - 1, *shape), jnp.bfloat16) for shape in blocks]
        block = [pltpu.VMEM(shape, jnp.bfloat16) for shape in blocks]
        moments = [pltpu.VMEM(shape, jnp.float32) for shape in blocks]
        scratch = [*per_step, *per_step, *hops, *block, *moments, *moments]
        one = dma((count,))
        semaphores = [
            dma((AHEAD, count)),
            dma((2 * AHEAD, count)),
            dma((len(FIRST) + 2,)),
            dma((chips, count)),
            dma((len(LAST) + 2,)),
            *[one] * 4,
        ]
        hbm, vmem = pl.BlockSpec(memory_space=pltpu.HBM), pl.BlockSpec(memory_space=pltpu.VMEM)
        shapes = [jax.ShapeDtypeStruct(w.shape, w.dtype) for w in weights] + [jax.ShapeDtypeStruct(b, jnp.float32) for b in blocks] * 2
        inside = pl.pallas_call(
            body,
            out_shape=[pltpu.VMEM(one.shape, one.dtype) for one in shapes],
            in_specs=[hbm] * len(arrays),
            out_specs=[vmem] * len(shapes),
            scratch_shapes=[*scratch, *semaphores],
            compiler_params=pltpu.CompilerParams(collective_id=0, has_side_effects=True, vmem_limit_bytes=SCRATCH_BYTES),
        )(*arrays)
        return pl.pallas_call(
            functools.partial(write_out, len(shapes)),
            out_shape=shapes,
            in_specs=[vmem] * len(shapes),
            out_specs=[hbm] * len(shapes),
            scratch_shapes=[dma((len(shapes),))],
            compiler_params=pltpu.CompilerParams(vmem_limit_bytes=WRITE_BYTES),
        )(*inside)

    all_of, shared = P(None, None, None), P(None, "dp", None)
    return jax.shard_map(
        step,
        mesh=mesh,
        in_specs=(P(("rep", "dp"), None, None, None),) * 3 + (all_of,) * 3 + (shared,) * 6,
        out_specs=(P("rep", None, None),) * 3 + (P("rep", "dp", None),) * 6,
        check_vma=False,
    )
```

```python
import functools

import jax
import jax.numpy as jnp
from jax import lax
from jax.experimental import pallas as pl
from jax.experimental.pallas import tpu as pltpu
from jax.sharding import PartitionSpec as P

MESH = pl.DeviceIdType.MESH
CORES = 2
AHEAD = 1
FIRST = (1,)
LAST = (3,)
TILE = 16
SCRATCH_BYTES = 43 << 20
WRITE_BYTES = 1 << 20


def adamw(w, m, v, g):
    m = 0.9 * m + 0.1 * g
    v = 0.95 * v + 0.05 * g * g
    step = m * lax.rsqrt(v + 1e-8) + 0.1 * w
    return (w - 0.02 * step).astype(jnp.bfloat16), m, v


def write_out(groups, layers, *refs):
    kinds, count = len(refs) // (len(groups) + sum(map(len, groups))), sum(map(len, groups))
    places, sem = refs[kinds * len(groups) : -1], refs[-1]
    copies = []
    for kind in range(kinds):
        for source, group in zip(refs[kind * len(groups) :], groups, strict=False):
            for k, i in enumerate(group):
                q = kind * count + i
                copies.append(pltpu.make_async_copy(source.at[pl.ds(k * layers, layers)], places[q], sem.at[q]))
    for copy in copies:
        copy.start()
    for copy in copies:
        copy.wait()


def cut(shape, sizes, backwards):
    layers, height = shape[:2]
    ends, at = [], 0
    for size in sizes:
        ends.append((at, at + size * TILE))
        at += size * TILE
    ends.append((at, height))
    if backwards:
        ends = [(height - high, height - low) for low, high in reversed(ends)]
        return [((0, layers - 1), (0, height)), *[((layers - 1, layers), one) for one in ends]]
    return [*[((0, 1), one) for one in ends], *[((l, l + 1), (0, height)) for l in range(1, layers)]]


def kernel(n, groups, layers, terms, weights, m_from, v_from, new, m_out, v_out, mine, theirs, partial, own_w, m_in, v_in, sems):
    mine_sem, take_sem, first_sem, hop_sem, end_sem, load_sem, chip_out, ring_out, fwd_in = sems
    chips = n // CORES
    last = chips - 1
    me = lax.axis_index("dp")
    chip, core = me // CORES, me % CORES
    way = 1 - CORES * core
    other = chip * CORES + (1 - core)
    shapes = [ref.shape[1:] for ref in mine]
    height = [shape[1] for shape in shapes]
    every = range(len(groups))
    whole = [[((0, shape[0]), (0, shape[1]))] for shape in shapes]
    first, opening, final = [*whole], [*whole], [*whole]
    first[0] = cut(shapes[0], FIRST, False)
    opening[0] = [((l, l + layers), (0, height[0])) for l in range(0, shapes[0][0], layers)]
    final[-1] = cut(shapes[-1], LAST, True)

    def device_at(steps, which):
        return lax.rem(chip + way * steps + chips, chips) * CORES + which

    onward, across = device_at(1, core), device_at(1, 1 - core)

    def remote(source, place, send_sem, recv_sem, device):
        return pltpu.make_async_remote_copy(
            src_ref=source, dst_ref=place, send_sem=send_sem, recv_sem=recv_sem, device_id={"dp": device}, device_id_type=MESH
        )

    def rows(g, device, part=None):
        low, high = part or (0, height[g])
        return pl.ds(pl.multiple_of(device * height[g] + low, TILE), high - low)

    def span(low, high):
        return pl.ds(low, high - low)

    def by_array(g, part):
        low, high = part[0]
        for k, i in enumerate(groups[g]):
            a, b = max(low, k * layers), min(high, (k + 1) * layers)
            if a < b:
                yield i, pl.ds(a - k * layers, b - a), pl.ds(a, b - a)

    def fetch(s, g):
        for i, inner, outer in by_array(g, whole[g][0]):
            source = terms[i].at[0, inner, rows(g, device_at(-1 - s, core))]
            pltpu.make_async_copy(source, mine[g].at[s, outer], mine_sem.at[s % AHEAD, g]).start()

    def fetched(s, g):
        pltpu.make_async_copy(mine[g].at[s], mine[g].at[s], mine_sem.at[s % AHEAD, g]).wait()

    def parts_of_sum(s, g):
        return first[g] if s == 0 else whole[g]

    def parts_of_new(s, g):
        return final[g] if s == last - 1 else opening[g] if s == 0 else whole[g]

    def take_at(s, g, k):
        return first_sem.at[k] if len(parts_of_sum(s, g)) > 1 else take_sem.at[s % (2 * AHEAD), g]

    def give(s):
        for g in every:
            for k, part in enumerate(parts_of_sum(s, g)):
                for i, inner, outer in by_array(g, part):
                    source = terms[i].at[0, inner, rows(g, device_at(1 + s, 1 - core), part[1])]
                    remote(source, theirs[g].at[s, outer, span(*part[1])], chip_out.at[g], take_at(s, g, k), other).start()

    def taken(s, g, k):
        piece, part = parts_of_sum(s, g)[k]
        place = theirs[g].at[s, span(*piece), span(*part)]
        remote(place, place, chip_out.at[g], take_at(s, g, k), other).wait_recv()

    def send_sum(s, g, k=None):
        piece, part = whole[g][0] if k is None else parts_of_sum(s, g)[k]
        source, place = (ref[g].at[s, span(*piece), span(*part)] for ref in (mine, partial))
        return remote(source, place, ring_out.at[g], hop_sem.at[s % chips, g], onward)

    def is_end(s, g, k):
        return s == last - 1 and g == every[-1] and k == len(final[g]) - 1

    def send_new(s, g, k=None):
        piece, part = whole[g][0] if k is None else parts_of_new(s, g)[k]
        block = new[g].at[span(*piece), rows(g, device_at(-s, core), part)]
        sem = end_sem.at[k] if s == last - 1 and len(final[g]) > 1 else hop_sem.at[(last + s) % chips, g]
        return remote(block, block, ring_out.at[g], sem, onward)

    def hand(s, g, k):
        send_new(s, g, k).start()
        if is_end(s, g, k):
            piece, part = parts_of_new(s, g)[k]
            block = new[g].at[span(*piece), rows(g, device_at(-s, core), part)]
            remote(block, block, chip_out.at[g], fwd_in.at[g], across).start()

    def forward(s, g, part):
        block = new[g].at[span(*part[0]), rows(g, device_at(-s, core), part[1])]
        remote(block, block, chip_out.at[g], fwd_in.at[g], other).start()

    barrier = pltpu.get_barrier_semaphore()
    near = (other, onward, device_at(-1, core), across)
    for device in near:
        pl.semaphore_signal(barrier, inc=1, device_id={"dp": device}, device_id_type=MESH)
    for g in every:
        fetch(0, g)
    pl.semaphore_wait(barrier, len(near))
    give(0)
    for s in range(1, AHEAD):
        for g in every:
            fetch(s, g)
        give(s)

    def over_tiles(g, part, do):
        for l in range(*part[0]):

            @pl.loop(part[1][0] // TILE, part[1][1] // TILE)
            def _(tile):
                do(g, l, tile, pl.ds(pl.multiple_of(tile * TILE, TILE), TILE))

    def total(s, g, l, at):
        one = mine[g][s, l, at].astype(jnp.float32) + theirs[g][s, l, at].astype(jnp.float32)
        if s > 0:
            one = one + partial[g][s - 1, l, at].astype(jnp.float32)
        return one.astype(jnp.bfloat16)

    for s in range(last):
        for g in every:
            fetched(s, g)
            if s > 0:
                send_sum(s - 1, g).wait_recv()
            for k, part in enumerate(parts_of_sum(s, g)):
                taken(s, g, k)

                def add(g, l, tile, at):
                    mine[g][s, l, at] = total(s, g, l, at)

                over_tiles(g, part, add)
                send_sum(s, g, k).start()
        if s + AHEAD < chips:
            for g in every:
                fetch(s + AHEAD, g)
            give(s + AHEAD)
        if s == 0:
            for g in every:
                for i, _, outer in by_array(g, whole[g][0]):
                    pltpu.make_async_copy(weights[i].at[:, rows(g, me)], own_w[g].at[outer], load_sem.at[g]).start()
                    pltpu.make_async_copy(m_from[i], m_in[g].at[outer], load_sem.at[g]).start()
                    pltpu.make_async_copy(v_from[i], v_in[g].at[outer], load_sem.at[g]).start()

    for g in every:
        five = theirs[g].at[pl.ds(0, 5)]
        pltpu.make_async_copy(five, five, load_sem.at[g]).wait()
        fetched(last, g)
        taken(last, g, 0)
        send_sum(last - 1, g).wait_recv()
        start = pl.multiple_of(me * height[g], TILE)

        def take_step(g, l, tile, at):
            one = total(last, g, l, at).astype(jnp.float32)
            w, m, v = adamw(own_w[g][l, at].astype(jnp.float32), m_in[g][l, at], v_in[g][l, at], one)
            new[g][l, pl.ds(pl.multiple_of(start + tile * TILE, TILE), TILE)] = w
            m_out[g][l, at] = m
            v_out[g][l, at] = v

        for k, part in enumerate(parts_of_new(0, g)):
            over_tiles(g, part, take_step)
            hand(0, g, k)
            forward(0, g, part)
    for s in range(1, chips):
        for g in every:
            came = parts_of_new(s - 1, g)
            if s == last and len(came) > 1:
                for k, part in enumerate(came):
                    send_new(s - 1, g, k).wait_recv()
                    if not is_end(s - 1, g, k):
                        forward(s, g, part)
                continue
            send_new(s - 1, g).wait_recv()
            if s < last:
                for k in range(len(parts_of_new(s, g))):
                    hand(s, g, k)
            forward(s, g, whole[g][0])
    for g in every:
        ring = new[g].at[:, pl.ds(0, 2 * last * height[g])]
        remote(ring, ring, ring_out.at[g], fwd_in.at[g], onward).wait_send()
        remote(new[g], new[g], chip_out.at[g], fwd_in.at[g], other).wait_send()
        half = new[g].at[:, pl.ds(0, chips * height[g])]
        remote(half, half, chip_out.at[g], fwd_in.at[g], other).wait_recv()


def solution(mesh):
    n = mesh.shape["dp"]
    chips = n // CORES

    def step(*arrays):
        terms, weights, m, v = (arrays[i : i + 3] for i in (0, 3, 6, 9))
        blocks = [one.shape for one in m]
        layers = blocks[0][0]
        groups = [[i for i, b in enumerate(blocks) if b == shape] for shape in dict.fromkeys(blocks)]
        count, kinds = len(groups), (terms, weights, m, v)
        inputs = sum(map(len, kinds))
        dma = pltpu.SemaphoreType.DMA

        def body(*refs):
            given = [refs[i : i + len(m)] for i in range(0, inputs, len(m))]
            made = [refs[i : i + count] for i in range(inputs, inputs + 9 * count, count)]
            kernel(n, groups, layers, *given, *made, refs[inputs + 9 * count :])

        block = [(layers * len(group), *blocks[group[0]][1:]) for group in groups]
        full = [(layers * len(group), *weights[group[0]].shape[1:]) for group in groups]
        per_step = [pltpu.VMEM((chips, *one), jnp.bfloat16) for one in block]
        hops = [pltpu.VMEM((chips - 1, *one), jnp.bfloat16) for one in block]
        moments = [pltpu.VMEM(one, jnp.float32) for one in block]
        scratch = [*per_step, *per_step, *hops, *(pltpu.VMEM(one, jnp.bfloat16) for one in block), *moments, *moments]
        one = dma((count,))
        semaphores = [
            dma((AHEAD, count)),
            dma((2 * AHEAD, count)),
            dma((len(FIRST) + block[0][0],)),
            dma((chips, count)),
            dma((len(LAST) + 2,)),
            *[one] * 4,
        ]
        hbm, vmem = pl.BlockSpec(memory_space=pltpu.HBM), pl.BlockSpec(memory_space=pltpu.VMEM)
        inside = pl.pallas_call(
            body,
            out_shape=[*(pltpu.VMEM(one, jnp.bfloat16) for one in full), *moments, *moments],
            in_specs=[hbm] * len(arrays),
            out_specs=[vmem] * (3 * count),
            scratch_shapes=[*scratch, *semaphores],
            compiler_params=pltpu.CompilerParams(collective_id=0, has_side_effects=True, vmem_limit_bytes=SCRATCH_BYTES),
        )(*arrays)
        shapes = [jax.ShapeDtypeStruct(w.shape, w.dtype) for w in weights] + [jax.ShapeDtypeStruct(b, jnp.float32) for b in blocks] * 2
        return pl.pallas_call(
            functools.partial(write_out, groups, layers),
            out_shape=shapes,
            in_specs=[vmem] * (3 * count),
            out_specs=[hbm] * len(shapes),
            scratch_shapes=[dma((len(shapes),))],
            compiler_params=pltpu.CompilerParams(vmem_limit_bytes=WRITE_BYTES),
        )(*inside)

    all_of, shared = P(None, None, None), P(None, "dp", None)
    return jax.shard_map(
        step,
        mesh=mesh,
        in_specs=(P(("rep", "dp"), None, None, None),) * 3 + (all_of,) * 3 + (shared,) * 6,
        out_specs=(P("rep", None, None),) * 3 + (P("rep", "dp", None),) * 6,
        check_vma=False,
    )
```

```python
import functools

import jax
import jax.numpy as jnp
from jax import lax
from jax.experimental import pallas as pl
from jax.experimental.pallas import tpu as pltpu
from jax.sharding import PartitionSpec as P

MESH = pl.DeviceIdType.MESH
CORES = 2
AHEAD = 1
FIRST = (1,)
LAST = (3,)
TILE = 16
SCRATCH_BYTES = 43 << 20
WRITE_BYTES = 1 << 20


def adamw(w, m, v, g):
    m = 0.9 * m + 0.1 * g
    v = 0.95 * v + 0.05 * g * g
    step = m * lax.rsqrt(v + 1e-8) + 0.1 * w
    return (w - 0.02 * step).astype(jnp.bfloat16), m, v


def write_out(groups, layers, *refs):
    kinds, count = len(refs) // (len(groups) + sum(map(len, groups))), sum(map(len, groups))
    places, sem = refs[kinds * len(groups) : -1], refs[-1]
    copies = []
    for kind in range(kinds):
        for source, group in zip(refs[kind * len(groups) :], groups, strict=False):
            for k, i in enumerate(group):
                q = kind * count + i
                copies.append(pltpu.make_async_copy(source.at[pl.ds(k * layers, layers)], places[q], sem.at[q]))
    for copy in copies:
        copy.start()
    for copy in copies:
        copy.wait()


def cut(shape, sizes, backwards):
    layers, height = shape[:2]
    ends, at = [], 0
    for size in sizes:
        ends.append((at, at + size * TILE))
        at += size * TILE
    ends.append((at, height))
    if backwards:
        ends = [(height - high, height - low) for low, high in reversed(ends)]
        return [((0, layers - 1), (0, height)), *[((layers - 1, layers), one) for one in ends]]
    return [*[((0, 1), one) for one in ends], *[((l, l + 1), (0, height)) for l in range(1, layers)]]


def kernel(n, groups, layers, terms, weights, m_from, v_from, new, m_out, v_out, mine, theirs, partial, own_w, m_in, v_in, sems):
    mine_sem, take_sem, first_sem, hop_sem, end_sem, load_sem, chip_out, ring_out, fwd_in = sems
    chips = n // CORES
    last = chips - 1
    me = lax.axis_index("dp")
    chip, core = me // CORES, me % CORES
    way = CORES * core - 1
    other = chip * CORES + (1 - core)
    shapes = [ref.shape[1:] for ref in mine]
    height = [shape[1] for shape in shapes]
    every = range(len(groups))
    whole = [[((0, shape[0]), (0, shape[1]))] for shape in shapes]
    first, opening, final = [*whole], [*whole], [*whole]
    first[0] = cut(shapes[0], FIRST, False)
    opening[0] = [((l, l + layers), (0, height[0])) for l in range(0, shapes[0][0], layers)]
    final[-1] = cut(shapes[-1], LAST, True)

    def device_at(steps, which):
        return lax.rem(chip + way * steps + chips, chips) * CORES + which

    onward, across = device_at(1, core), device_at(1, 1 - core)

    def remote(source, place, send_sem, recv_sem, device):
        return pltpu.make_async_remote_copy(
            src_ref=source, dst_ref=place, send_sem=send_sem, recv_sem=recv_sem, device_id={"dp": device}, device_id_type=MESH
        )

    def rows(g, device, part=None):
        low, high = part or (0, height[g])
        return pl.ds(pl.multiple_of(device * height[g] + low, TILE), high - low)

    def span(low, high):
        return pl.ds(low, high - low)

    def by_array(g, part):
        low, high = part[0]
        for k, i in enumerate(groups[g]):
            a, b = max(low, k * layers), min(high, (k + 1) * layers)
            if a < b:
                yield i, pl.ds(a - k * layers, b - a), pl.ds(a, b - a)

    def fetch(s, g):
        for i, inner, outer in by_array(g, whole[g][0]):
            source = terms[i].at[0, inner, rows(g, device_at(-1 - s, core))]
            pltpu.make_async_copy(source, mine[g].at[s, outer], mine_sem.at[s % AHEAD, g]).start()

    def fetched(s, g):
        pltpu.make_async_copy(mine[g].at[s], mine[g].at[s], mine_sem.at[s % AHEAD, g]).wait()

    def parts_of_sum(s, g):
        return first[g] if s == 0 else whole[g]

    def parts_of_new(s, g):
        return final[g] if s == last - 1 else opening[g] if s == 0 else whole[g]

    def take_at(s, g, k):
        return first_sem.at[k] if len(parts_of_sum(s, g)) > 1 else take_sem.at[s % (2 * AHEAD), g]

    def give(s):
        for g in every:
            for k, part in enumerate(parts_of_sum(s, g)):
                for i, inner, outer in by_array(g, part):
                    source = terms[i].at[0, inner, rows(g, device_at(1 + s, 1 - core), part[1])]
                    remote(source, theirs[g].at[s, outer, span(*part[1])], chip_out.at[g], take_at(s, g, k), other).start()

    def taken(s, g, k):
        piece, part = parts_of_sum(s, g)[k]
        place = theirs[g].at[s, span(*piece), span(*part)]
        remote(place, place, chip_out.at[g], take_at(s, g, k), other).wait_recv()

    def send_sum(s, g, k=None):
        piece, part = whole[g][0] if k is None else parts_of_sum(s, g)[k]
        source, place = (ref[g].at[s, span(*piece), span(*part)] for ref in (mine, partial))
        return remote(source, place, ring_out.at[g], hop_sem.at[s % chips, g], onward)

    def is_end(s, g, k):
        return s == last - 1 and g == every[-1] and k == len(final[g]) - 1

    def send_new(s, g, k=None):
        piece, part = whole[g][0] if k is None else parts_of_new(s, g)[k]
        block = new[g].at[span(*piece), rows(g, device_at(-s, core), part)]
        sem = end_sem.at[k] if s == last - 1 and len(final[g]) > 1 else hop_sem.at[(last + s) % chips, g]
        return remote(block, block, ring_out.at[g], sem, onward)

    def hand(s, g, k):
        send_new(s, g, k).start()
        if is_end(s, g, k):
            piece, part = parts_of_new(s, g)[k]
            block = new[g].at[span(*piece), rows(g, device_at(-s, core), part)]
            remote(block, block, chip_out.at[g], fwd_in.at[g], across).start()

    def forward(s, g, part):
        block = new[g].at[span(*part[0]), rows(g, device_at(-s, core), part[1])]
        remote(block, block, chip_out.at[g], fwd_in.at[g], other).start()

    barrier = pltpu.get_barrier_semaphore()
    near = (other, onward, device_at(-1, core), across)
    for device in near:
        pl.semaphore_signal(barrier, inc=1, device_id={"dp": device}, device_id_type=MESH)
    for g in every:
        fetch(0, g)
    pl.semaphore_wait(barrier, len(near))
    give(0)
    for s in range(1, AHEAD):
        for g in every:
            fetch(s, g)
        give(s)

    def over_tiles(g, part, do):
        for l in range(*part[0]):

            @pl.loop(part[1][0] // TILE, part[1][1] // TILE)
            def _(tile):
                do(g, l, tile, pl.ds(pl.multiple_of(tile * TILE, TILE), TILE))

    def total(s, g, l, at):
        one = mine[g][s, l, at].astype(jnp.float32) + theirs[g][s, l, at].astype(jnp.float32)
        if s > 0:
            one = one + partial[g][s - 1, l, at].astype(jnp.float32)
        return one.astype(jnp.bfloat16)

    for s in range(last):
        for g in every:
            fetched(s, g)
            if s > 0:
                send_sum(s - 1, g).wait_recv()
            for k, part in enumerate(parts_of_sum(s, g)):
                taken(s, g, k)

                def add(g, l, tile, at):
                    mine[g][s, l, at] = total(s, g, l, at)

                over_tiles(g, part, add)
                send_sum(s, g, k).start()
        if s + AHEAD < chips:
            for g in every:
                fetch(s + AHEAD, g)
            give(s + AHEAD)
        if s == 0:
            for g in every:
                for i, _, outer in by_array(g, whole[g][0]):
                    pltpu.make_async_copy(weights[i].at[:, rows(g, me)], own_w[g].at[outer], load_sem.at[g]).start()
                    pltpu.make_async_copy(m_from[i], m_in[g].at[outer], load_sem.at[g]).start()
                    pltpu.make_async_copy(v_from[i], v_in[g].at[outer], load_sem.at[g]).start()

    for g in every:
        five = theirs[g].at[pl.ds(0, 5)]
        pltpu.make_async_copy(five, five, load_sem.at[g]).wait()
        fetched(last, g)
        taken(last, g, 0)
        send_sum(last - 1, g).wait_recv()
        start = pl.multiple_of(me * height[g], TILE)

        def take_step(g, l, tile, at):
            one = total(last, g, l, at).astype(jnp.float32)
            w, m, v = adamw(own_w[g][l, at].astype(jnp.float32), m_in[g][l, at], v_in[g][l, at], one)
            new[g][l, pl.ds(pl.multiple_of(start + tile * TILE, TILE), TILE)] = w
            m_out[g][l, at] = m
            v_out[g][l, at] = v

        for k, part in enumerate(parts_of_new(0, g)):
            over_tiles(g, part, take_step)
            hand(0, g, k)
            forward(0, g, part)
    for s in range(1, chips):
        for g in every:
            came = parts_of_new(s - 1, g)
            if s == last and len(came) > 1:
                for k, part in enumerate(came):
                    send_new(s - 1, g, k).wait_recv()
                    if not is_end(s - 1, g, k):
                        forward(s, g, part)
                continue
            send_new(s - 1, g).wait_recv()
            if s < last:
                for k in range(len(parts_of_new(s, g))):
                    hand(s, g, k)
            forward(s, g, whole[g][0])
    for g in every:
        ring = new[g].at[:, pl.ds(0, 2 * last * height[g])]
        remote(ring, ring, ring_out.at[g], fwd_in.at[g], onward).wait_send()
        remote(new[g], new[g], chip_out.at[g], fwd_in.at[g], other).wait_send()
        half = new[g].at[:, pl.ds(0, chips * height[g])]
        remote(half, half, chip_out.at[g], fwd_in.at[g], other).wait_recv()


def solution(mesh):
    n = mesh.shape["dp"]
    chips = n // CORES

    def step(*arrays):
        terms, weights, m, v = (arrays[i : i + 3] for i in (0, 3, 6, 9))
        blocks = [one.shape for one in m]
        layers = blocks[0][0]
        groups = [[i for i, b in enumerate(blocks) if b == shape] for shape in dict.fromkeys(blocks)]
        count, kinds = len(groups), (terms, weights, m, v)
        inputs = sum(map(len, kinds))
        dma = pltpu.SemaphoreType.DMA

        def body(*refs):
            given = [refs[i : i + len(m)] for i in range(0, inputs, len(m))]
            made = [refs[i : i + count] for i in range(inputs, inputs + 9 * count, count)]
            kernel(n, groups, layers, *given, *made, refs[inputs + 9 * count :])

        block = [(layers * len(group), *blocks[group[0]][1:]) for group in groups]
        full = [(layers * len(group), *weights[group[0]].shape[1:]) for group in groups]
        per_step = [pltpu.VMEM((chips, *one), jnp.bfloat16) for one in block]
        hops = [pltpu.VMEM((chips - 1, *one), jnp.bfloat16) for one in block]
        moments = [pltpu.VMEM(one, jnp.float32) for one in block]
        scratch = [*per_step, *per_step, *hops, *(pltpu.VMEM(one, jnp.bfloat16) for one in block), *moments, *moments]
        one = dma((count,))
        semaphores = [
            dma((AHEAD, count)),
            dma((2 * AHEAD, count)),
            dma((len(FIRST) + block[0][0],)),
            dma((chips, count)),
            dma((len(LAST) + 2,)),
            *[one] * 4,
        ]
        hbm, vmem = pl.BlockSpec(memory_space=pltpu.HBM), pl.BlockSpec(memory_space=pltpu.VMEM)
        inside = pl.pallas_call(
            body,
            out_shape=[*(pltpu.VMEM(one, jnp.bfloat16) for one in full), *moments, *moments],
            in_specs=[hbm] * len(arrays),
            out_specs=[vmem] * (3 * count),
            scratch_shapes=[*scratch, *semaphores],
            compiler_params=pltpu.CompilerParams(collective_id=0, has_side_effects=True, vmem_limit_bytes=SCRATCH_BYTES),
        )(*arrays)
        shapes = [jax.ShapeDtypeStruct(w.shape, w.dtype) for w in weights] + [jax.ShapeDtypeStruct(b, jnp.float32) for b in blocks] * 2
        return pl.pallas_call(
            functools.partial(write_out, groups, layers),
            out_shape=shapes,
            in_specs=[vmem] * (3 * count),
            out_specs=[hbm] * len(shapes),
            scratch_shapes=[dma((len(shapes),))],
            compiler_params=pltpu.CompilerParams(vmem_limit_bytes=WRITE_BYTES),
        )(*inside)

    all_of, shared = P(None, None, None), P(None, "dp", None)
    return jax.shard_map(
        step,
        mesh=mesh,
        in_specs=(P(("rep", "dp"), None, None, None),) * 3 + (all_of,) * 3 + (shared,) * 6,
        out_specs=(P("rep", None, None),) * 3 + (P("rep", "dp", None),) * 6,
        check_vma=False,
    )
```

```python
import functools

import jax
import jax.numpy as jnp
from jax import lax
from jax.experimental import pallas as pl
from jax.experimental.pallas import tpu as pltpu
from jax.sharding import PartitionSpec as P

MESH = pl.DeviceIdType.MESH
CORES = 2
AHEAD = 1
FIRST = (1,)
LAST = (3, 3)
TILE = 16
SCRATCH_BYTES = 43 << 20
WRITE_BYTES = 1 << 20


def adamw(w, m, v, g):
    m = 0.9 * m + 0.1 * g
    v = 0.95 * v + 0.05 * g * g
    step = m * lax.rsqrt(v + 1e-8) + 0.1 * w
    return (w - 0.02 * step).astype(jnp.bfloat16), m, v


def write_out(groups, layers, *refs):
    kinds, count = len(refs) // (len(groups) + sum(map(len, groups))), sum(map(len, groups))
    places, sem = refs[kinds * len(groups) : -1], refs[-1]
    for kind in range(kinds):
        for g, group in enumerate(groups):
            a = kind * len(groups) + g
            for k, i in enumerate(group):
                pltpu.make_async_copy(refs[a].at[pl.ds(k * layers, layers)], places[kind * count + i], sem.at[a]).start()
    for a in range(kinds * len(groups)):
        pltpu.make_async_copy(refs[a], refs[a], sem.at[a]).wait()


def cut(shape, sizes, backwards):
    layers, height = shape[:2]
    ends, at = [], 0
    for size in sizes:
        ends.append((at, at + size * TILE))
        at += size * TILE
    ends.append((at, height))
    if backwards:
        ends = [(height - high, height - low) for low, high in reversed(ends)]
        return [((0, layers - 1), (0, height)), *[((layers - 1, layers), one) for one in ends]]
    return [*[((0, 1), one) for one in ends], ((1, layers), (0, height))]


def kernel(n, groups, layers, terms, weights, m_from, v_from, new, m_out, v_out, mine, theirs, partial, own_w, m_in, v_in, sems):
    mine_sem, take_sem, first_sem, hop_sem, end_sem, load_sem, chip_out, ring_out, fwd_in = sems
    chips = n // CORES
    last = chips - 1
    me = lax.axis_index("dp")
    chip, core = me // CORES, me % CORES
    way = CORES * core - 1
    other = chip * CORES + (1 - core)
    shapes = [ref.shape[1:] for ref in mine]
    height = [shape[1] for shape in shapes]
    every = range(len(groups))
    whole = [[((0, shape[0]), (0, shape[1]))] for shape in shapes]
    first, opening, final = [*whole], [*whole], [*whole]
    first[0] = cut(shapes[0], FIRST, False)
    opening[0] = [((l, l + layers), (0, height[0])) for l in range(0, shapes[0][0], layers)]
    final[-1] = cut(shapes[-1], LAST, True)

    def device_at(steps, which):
        return lax.rem(chip + way * steps + chips, chips) * CORES + which

    onward, across = device_at(1, core), device_at(1, 1 - core)

    def remote(source, place, send_sem, recv_sem, device):
        return pltpu.make_async_remote_copy(
            src_ref=source, dst_ref=place, send_sem=send_sem, recv_sem=recv_sem, device_id={"dp": device}, device_id_type=MESH
        )

    def rows(g, device, part=None):
        low, high = part or (0, height[g])
        return pl.ds(pl.multiple_of(device * height[g] + low, TILE), high - low)

    def span(low, high):
        return pl.ds(low, high - low)

    def by_array(g, part):
        low, high = part[0]
        for k, i in enumerate(groups[g]):
            a, b = max(low, k * layers), min(high, (k + 1) * layers)
            if a < b:
                yield i, pl.ds(a - k * layers, b - a), pl.ds(a, b - a)

    def fetch(s, g):
        for i, inner, outer in by_array(g, whole[g][0]):
            source = terms[i].at[0, inner, rows(g, device_at(-1 - s, core))]
            pltpu.make_async_copy(source, mine[g].at[s, outer], mine_sem.at[s % AHEAD, g]).start()

    def fetched(s, g):
        pltpu.make_async_copy(mine[g].at[s], mine[g].at[s], mine_sem.at[s % AHEAD, g]).wait()

    def parts_of_sum(s, g):
        return first[g] if s == 0 else whole[g]

    def parts_of_new(s, g):
        return final[g] if s == last - 1 else opening[g] if s == 0 else whole[g]

    def take_at(s, g, k):
        return first_sem.at[k] if len(parts_of_sum(s, g)) > 1 else take_sem.at[s % (2 * AHEAD), g]

    def give(s):
        for g in every:
            for k, part in enumerate(parts_of_sum(s, g)):
                for i, inner, outer in by_array(g, part):
                    source = terms[i].at[0, inner, rows(g, device_at(1 + s, 1 - core), part[1])]
                    remote(source, theirs[g].at[s, outer, span(*part[1])], chip_out.at[g], take_at(s, g, k), other).start()

    def taken(s, g, k):
        piece, part = parts_of_sum(s, g)[k]
        place = theirs[g].at[s, span(*piece), span(*part)]
        remote(place, place, chip_out.at[g], take_at(s, g, k), other).wait_recv()

    def send_sum(s, g, k=None):
        piece, part = whole[g][0] if k is None else parts_of_sum(s, g)[k]
        source, place = (ref[g].at[s, span(*piece), span(*part)] for ref in (mine, partial))
        return remote(source, place, ring_out.at[g], hop_sem.at[s % chips, g], onward)

    def is_end(s, g, k):
        return s == last - 1 and g == every[-1] and k == len(final[g]) - 1

    def send_new(s, g, k=None):
        piece, part = whole[g][0] if k is None else parts_of_new(s, g)[k]
        block = new[g].at[span(*piece), rows(g, device_at(-s, core), part)]
        sem = end_sem.at[k] if s == last - 1 and len(final[g]) > 1 else hop_sem.at[(last + s) % chips, g]
        return remote(block, block, ring_out.at[g], sem, onward)

    def hand(s, g, k):
        send_new(s, g, k).start()
        if is_end(s, g, k):
            piece, part = parts_of_new(s, g)[k]
            block = new[g].at[span(*piece), rows(g, device_at(-s, core), part)]
            remote(block, block, chip_out.at[g], fwd_in.at[g], across).start()

    def forward(s, g, part):
        block = new[g].at[span(*part[0]), rows(g, device_at(-s, core), part[1])]
        remote(block, block, chip_out.at[g], fwd_in.at[g], other).start()

    barrier = pltpu.get_barrier_semaphore()
    near = (onward, device_at(-1, core), across, other)
    for device in near:
        pl.semaphore_signal(barrier, inc=1, device_id={"dp": device}, device_id_type=MESH)
    for g in every:
        fetch(0, g)
    pl.semaphore_wait(barrier, len(near))
    give(0)
    for s in range(1, AHEAD):
        for g in every:
            fetch(s, g)
        give(s)

    def over_tiles(g, part, do):
        for l in range(*part[0]):

            @pl.loop(part[1][0] // TILE, part[1][1] // TILE)
            def _(tile):
                do(g, l, tile, pl.ds(pl.multiple_of(tile * TILE, TILE), TILE))

    def total(s, g, l, at):
        one = mine[g][s, l, at].astype(jnp.float32) + theirs[g][s, l, at].astype(jnp.float32)
        if s > 0:
            one = one + partial[g][s - 1, l, at].astype(jnp.float32)
        return one.astype(jnp.bfloat16)

    for s in range(last):
        for g in every:
            fetched(s, g)
            if s > 0:
                send_sum(s - 1, g).wait_recv()
            for k, part in enumerate(parts_of_sum(s, g)):
                taken(s, g, k)

                def add(g, l, tile, at):
                    mine[g][s, l, at] = total(s, g, l, at)

                over_tiles(g, part, add)
                send_sum(s, g, k).start()
        if s + AHEAD < chips:
            for g in every:
                fetch(s + AHEAD, g)
            give(s + AHEAD)
        if s == 0:
            for g in every:
                for i, _, outer in by_array(g, whole[g][0]):
                    pltpu.make_async_copy(weights[i].at[:, rows(g, me)], own_w[g].at[outer], load_sem.at[g]).start()
                    pltpu.make_async_copy(m_from[i], m_in[g].at[outer], load_sem.at[g]).start()
                    pltpu.make_async_copy(v_from[i], v_in[g].at[outer], load_sem.at[g]).start()

    for g in every:
        five = theirs[g].at[pl.ds(0, 5)]
        pltpu.make_async_copy(five, five, load_sem.at[g]).wait()
        fetched(last, g)
        taken(last, g, 0)
        send_sum(last - 1, g).wait_recv()
        start = pl.multiple_of(me * height[g], TILE)

        def take_step(g, l, tile, at):
            one = total(last, g, l, at).astype(jnp.float32)
            w, m, v = adamw(own_w[g][l, at].astype(jnp.float32), m_in[g][l, at], v_in[g][l, at], one)
            new[g][l, pl.ds(pl.multiple_of(start + tile * TILE, TILE), TILE)] = w
            m_out[g][l, at] = m
            v_out[g][l, at] = v

        for k, part in enumerate(parts_of_new(0, g)):
            over_tiles(g, part, take_step)
            hand(0, g, k)
            forward(0, g, part)
    for s in range(1, chips):
        for g in every:
            came = parts_of_new(s - 1, g)
            if s == last and len(came) > 1:
                for k, part in enumerate(came):
                    send_new(s - 1, g, k).wait_recv()
                    if not is_end(s - 1, g, k):
                        forward(s, g, part)
                continue
            send_new(s - 1, g).wait_recv()
            if s < last:
                for k in range(len(parts_of_new(s, g))):
                    hand(s, g, k)
            forward(s, g, whole[g][0])
    for g in every:
        ring = new[g].at[:, pl.ds(0, 2 * last * height[g])]
        remote(ring, ring, ring_out.at[g], fwd_in.at[g], onward).wait_send()
        remote(new[g], new[g], chip_out.at[g], fwd_in.at[g], other).wait_send()
        half = new[g].at[:, pl.ds(0, chips * height[g])]
        remote(half, half, chip_out.at[g], fwd_in.at[g], other).wait_recv()


def solution(mesh):
    n = mesh.shape["dp"]
    chips = n // CORES

    def step(*arrays):
        terms, weights, m, v = (arrays[i : i + 3] for i in (0, 3, 6, 9))
        blocks = [one.shape for one in m]
        layers = blocks[0][0]
        groups = [[i for i, b in enumerate(blocks) if b == shape] for shape in dict.fromkeys(blocks)]
        count, kinds = len(groups), (terms, weights, m, v)
        inputs = sum(map(len, kinds))
        dma = pltpu.SemaphoreType.DMA

        def body(*refs):
            given = [refs[i : i + len(m)] for i in range(0, inputs, len(m))]
            made = [refs[i : i + count] for i in range(inputs, inputs + 9 * count, count)]
            kernel(n, groups, layers, *given, *made, refs[inputs + 9 * count :])

        block = [(layers * len(group), *blocks[group[0]][1:]) for group in groups]
        full = [(layers * len(group), *weights[group[0]].shape[1:]) for group in groups]
        per_step = [pltpu.VMEM((chips, *one), jnp.bfloat16) for one in block]
        hops = [pltpu.VMEM((chips - 1, *one), jnp.bfloat16) for one in block]
        moments = [pltpu.VMEM(one, jnp.float32) for one in block]
        scratch = [*per_step, *per_step, *hops, *(pltpu.VMEM(one, jnp.bfloat16) for one in block), *moments, *moments]
        one = dma((count,))
        semaphores = [
            dma((AHEAD, count)),
            dma((2 * AHEAD, count)),
            dma((len(FIRST) + 2,)),
            dma((chips, count)),
            dma((len(LAST) + 2,)),
            *[one] * 4,
        ]
        hbm, vmem = pl.BlockSpec(memory_space=pltpu.HBM), pl.BlockSpec(memory_space=pltpu.VMEM)
        inside = pl.pallas_call(
            body,
            out_shape=[*(pltpu.VMEM(one, jnp.bfloat16) for one in full), *moments, *moments],
            in_specs=[hbm] * len(arrays),
            out_specs=[vmem] * (3 * count),
            scratch_shapes=[*scratch, *semaphores],
            compiler_params=pltpu.CompilerParams(collective_id=0, has_side_effects=True, vmem_limit_bytes=SCRATCH_BYTES),
        )(*arrays)
        shapes = [jax.ShapeDtypeStruct(w.shape, w.dtype) for w in weights] + [jax.ShapeDtypeStruct(b, jnp.float32) for b in blocks] * 2
        return pl.pallas_call(
            functools.partial(write_out, groups, layers),
            out_shape=shapes,
            in_specs=[vmem] * (3 * count),
            out_specs=[hbm] * len(shapes),
            scratch_shapes=[dma((3 * count,))],
            compiler_params=pltpu.CompilerParams(vmem_limit_bytes=WRITE_BYTES),
        )(*inside)

    all_of, shared = P(None, None, None), P(None, "dp", None)
    return jax.shard_map(
        step,
        mesh=mesh,
        in_specs=(P(("rep", "dp"), None, None, None),) * 3 + (all_of,) * 3 + (shared,) * 6,
        out_specs=(P("rep", None, None),) * 3 + (P("rep", "dp", None),) * 6,
        check_vma=False,
    )
```

```python
import functools

import jax
import jax.numpy as jnp
from jax import lax
from jax.experimental import pallas as pl
from jax.experimental.pallas import tpu as pltpu
from jax.sharding import PartitionSpec as P

MESH = pl.DeviceIdType.MESH
CORES = 2
AHEAD = 1
FIRST = (1,)
LAST = (3, 3)
TILE = 16
SCRATCH_BYTES = 43 << 20
WRITE_BYTES = 1 << 20


def adamw(w, m, v, g):
    m = 0.9 * m + 0.1 * g
    v = 0.95 * v + 0.05 * g * g
    step = m * lax.rsqrt(v + 1e-8) + 0.1 * w
    return (w - 0.02 * step).astype(jnp.bfloat16), m, v


def write_out(groups, layers, *refs):
    kinds, count = len(refs) // (len(groups) + sum(map(len, groups))), sum(map(len, groups))
    places, sem = refs[kinds * len(groups) : -1], refs[-1]
    for kind in range(kinds):
        for g, group in enumerate(groups):
            a = kind * len(groups) + g
            for k, i in enumerate(group):
                pltpu.make_async_copy(refs[a].at[pl.ds(k * layers, layers)], places[kind * count + i], sem.at[a]).start()
    for a in range(kinds * len(groups)):
        pltpu.make_async_copy(refs[a], refs[a], sem.at[a]).wait()


def cut(shape, sizes, backwards):
    layers, height = shape[:2]
    ends, at = [], 0
    for size in sizes:
        ends.append((at, at + size * TILE))
        at += size * TILE
    ends.append((at, height))
    if backwards:
        ends = [(height - high, height - low) for low, high in reversed(ends)]
        return [((0, layers - 1), (0, height)), *[((layers - 1, layers), one) for one in ends]]
    return [*[((0, 1), one) for one in ends], ((1, layers), (0, height))]


def kernel(n, groups, layers, terms, weights, m_from, v_from, new, m_out, v_out, mine, theirs, partial, own_w, m_in, v_in, sems):
    mine_sem, take_sem, first_sem, hop_sem, end_sem, chip_out, ring_out, fwd_in = sems
    load_sem = first_sem
    chips = n // CORES
    last = chips - 1
    me = lax.axis_index("dp")
    chip, core = me // CORES, me % CORES
    way = CORES * core - 1
    other = chip * CORES + (1 - core)
    shapes = [ref.shape[1:] for ref in mine]
    height = [shape[1] for shape in shapes]
    every = range(len(groups))
    whole = [[((0, shape[0]), (0, shape[1]))] for shape in shapes]
    first, opening, final = [*whole], [*whole], [*whole]
    first[0] = cut(shapes[0], FIRST, False)
    opening[0] = [((l, l + layers), (0, height[0])) for l in range(0, shapes[0][0], layers)]
    final[-1] = cut(shapes[-1], LAST, True)

    def device_at(steps, which):
        return lax.rem(chip + way * steps + chips, chips) * CORES + which

    onward, across = device_at(1, core), device_at(1, 1 - core)

    def remote(source, place, send_sem, recv_sem, device):
        return pltpu.make_async_remote_copy(
            src_ref=source, dst_ref=place, send_sem=send_sem, recv_sem=recv_sem, device_id={"dp": device}, device_id_type=MESH
        )

    def rows(g, device, part=None):
        low, high = part or (0, height[g])
        return pl.ds(pl.multiple_of(device * height[g] + low, TILE), high - low)

    def span(low, high):
        return pl.ds(low, high - low)

    def by_array(g, part):
        low, high = part[0]
        for k, i in enumerate(groups[g]):
            a, b = max(low, k * layers), min(high, (k + 1) * layers)
            if a < b:
                yield i, pl.ds(a - k * layers, b - a), pl.ds(a, b - a)

    def fetch(s, g):
        for i, inner, outer in by_array(g, whole[g][0]):
            source = terms[i].at[0, inner, rows(g, device_at(-1 - s, core))]
            pltpu.make_async_copy(source, mine[g].at[s, outer], mine_sem.at[s % AHEAD, g]).start()

    def fetched(s, g):
        pltpu.make_async_copy(mine[g].at[s], mine[g].at[s], mine_sem.at[s % AHEAD, g]).wait()

    def parts_of_sum(s, g):
        return first[g] if s == 0 else whole[g]

    def parts_of_new(s, g):
        return final[g] if s == last - 1 else opening[g] if s == 0 else whole[g]

    def take_at(s, g, k):
        return first_sem.at[k] if len(parts_of_sum(s, g)) > 1 else take_sem.at[s % (2 * AHEAD), g]

    def give(s):
        for g in every:
            for k, part in enumerate(parts_of_sum(s, g)):
                for i, inner, outer in by_array(g, part):
                    source = terms[i].at[0, inner, rows(g, device_at(1 + s, 1 - core), part[1])]
                    remote(source, theirs[g].at[s, outer, span(*part[1])], chip_out.at[g], take_at(s, g, k), other).start()

    def taken(s, g, k):
        piece, part = parts_of_sum(s, g)[k]
        place = theirs[g].at[s, span(*piece), span(*part)]
        remote(place, place, chip_out.at[g], take_at(s, g, k), other).wait_recv()

    def send_sum(s, g, k=None):
        piece, part = whole[g][0] if k is None else parts_of_sum(s, g)[k]
        source, place = (ref[g].at[s, span(*piece), span(*part)] for ref in (mine, partial))
        return remote(source, place, ring_out.at[g], hop_sem.at[s % chips, g], onward)

    def is_end(s, g, k):
        return s == last - 1 and g == every[-1] and k == len(final[g]) - 1

    def send_new(s, g, k=None):
        piece, part = whole[g][0] if k is None else parts_of_new(s, g)[k]
        block = new[g].at[span(*piece), rows(g, device_at(-s, core), part)]
        sem = end_sem.at[k] if s == last - 1 and len(final[g]) > 1 else hop_sem.at[(last + s) % chips, g]
        return remote(block, block, ring_out.at[g], sem, onward)

    def hand(s, g, k):
        send_new(s, g, k).start()
        if is_end(s, g, k):
            piece, part = parts_of_new(s, g)[k]
            block = new[g].at[span(*piece), rows(g, device_at(-s, core), part)]
            remote(block, block, chip_out.at[g], fwd_in.at[g], across).start()

    def forward(s, g, part):
        block = new[g].at[span(*part[0]), rows(g, device_at(-s, core), part[1])]
        remote(block, block, chip_out.at[g], fwd_in.at[g], other).start()

    barrier = pltpu.get_barrier_semaphore()
    near = (onward, device_at(-1, core), across, other)
    for device in near:
        pl.semaphore_signal(barrier, inc=1, device_id={"dp": device}, device_id_type=MESH)
    for g in every:
        fetch(0, g)
    pl.semaphore_wait(barrier, len(near))
    give(0)
    for s in range(1, AHEAD):
        for g in every:
            fetch(s, g)
        give(s)

    def over_tiles(g, part, do):
        for l in range(*part[0]):

            @pl.loop(part[1][0] // TILE, part[1][1] // TILE)
            def _(tile):
                do(g, l, tile, pl.ds(pl.multiple_of(tile * TILE, TILE), TILE))

    def total(s, g, l, at):
        one = mine[g][s, l, at].astype(jnp.float32) + theirs[g][s, l, at].astype(jnp.float32)
        if s > 0:
            one = one + partial[g][s - 1, l, at].astype(jnp.float32)
        return one.astype(jnp.bfloat16)

    for s in range(last):
        for g in every:
            fetched(s, g)
            if s > 0:
                send_sum(s - 1, g).wait_recv()
            for k, part in enumerate(parts_of_sum(s, g)):
                taken(s, g, k)

                def add(g, l, tile, at):
                    mine[g][s, l, at] = total(s, g, l, at)

                over_tiles(g, part, add)
                send_sum(s, g, k).start()
        if s + AHEAD < chips:
            for g in every:
                fetch(s + AHEAD, g)
            give(s + AHEAD)
        if s == 0:
            for g in every:
                for i, _, outer in by_array(g, whole[g][0]):
                    pltpu.make_async_copy(weights[i].at[:, rows(g, me)], own_w[g].at[outer], load_sem.at[g]).start()
                    pltpu.make_async_copy(m_from[i], m_in[g].at[outer], load_sem.at[g]).start()
                    pltpu.make_async_copy(v_from[i], v_in[g].at[outer], load_sem.at[g]).start()

    for g in every:
        five = theirs[g].at[pl.ds(0, 5)]
        pltpu.make_async_copy(five, five, load_sem.at[g]).wait()
        fetched(last, g)
        taken(last, g, 0)
        send_sum(last - 1, g).wait_recv()
        start = pl.multiple_of(me * height[g], TILE)

        def take_step(g, l, tile, at):
            one = total(last, g, l, at).astype(jnp.float32)
            w, m, v = adamw(own_w[g][l, at].astype(jnp.float32), m_in[g][l, at], v_in[g][l, at], one)
            new[g][l, pl.ds(pl.multiple_of(start + tile * TILE, TILE), TILE)] = w
            m_out[g][l, at] = m
            v_out[g][l, at] = v

        for k, part in enumerate(parts_of_new(0, g)):
            over_tiles(g, part, take_step)
            hand(0, g, k)
            forward(0, g, part)
    for s in range(1, chips):
        for g in every:
            came = parts_of_new(s - 1, g)
            if s == last and len(came) > 1:
                for k, part in enumerate(came):
                    send_new(s - 1, g, k).wait_recv()
                    if not is_end(s - 1, g, k):
                        forward(s, g, part)
                continue
            send_new(s - 1, g).wait_recv()
            if s < last:
                for k in range(len(parts_of_new(s, g))):
                    hand(s, g, k)
            forward(s, g, whole[g][0])
    for g in every:
        ring = new[g].at[:, pl.ds(0, 2 * last * height[g])]
        remote(ring, ring, ring_out.at[g], fwd_in.at[g], onward).wait_send()
        remote(new[g], new[g], chip_out.at[g], fwd_in.at[g], other).wait_send()
        half = new[g].at[:, pl.ds(0, chips * height[g])]
        remote(half, half, chip_out.at[g], fwd_in.at[g], other).wait_recv()


def solution(mesh):
    n = mesh.shape["dp"]
    chips = n // CORES

    def step(*arrays):
        terms, weights, m, v = (arrays[i : i + 3] for i in (0, 3, 6, 9))
        blocks = [one.shape for one in m]
        layers = blocks[0][0]
        groups = [[i for i, b in enumerate(blocks) if b == shape] for shape in dict.fromkeys(blocks)]
        count, kinds = len(groups), (terms, weights, m, v)
        inputs = sum(map(len, kinds))
        dma = pltpu.SemaphoreType.DMA

        def body(*refs):
            given = [refs[i : i + len(m)] for i in range(0, inputs, len(m))]
            made = [refs[i : i + count] for i in range(inputs, inputs + 9 * count, count)]
            kernel(n, groups, layers, *given, *made, refs[inputs + 9 * count :])

        block = [(layers * len(group), *blocks[group[0]][1:]) for group in groups]
        full = [(layers * len(group), *weights[group[0]].shape[1:]) for group in groups]
        per_step = [pltpu.VMEM((chips, *one), jnp.bfloat16) for one in block]
        hops = [pltpu.VMEM((chips - 1, *one), jnp.bfloat16) for one in block]
        moments = [pltpu.VMEM(one, jnp.float32) for one in block]
        scratch = [*per_step, *per_step, *hops, *(pltpu.VMEM(one, jnp.bfloat16) for one in block), *moments, *moments]
        one = dma((count,))
        semaphores = [
            dma((AHEAD, count)),
            dma((2 * AHEAD, count)),
            dma((len(FIRST) + 2,)),
            dma((chips, count)),
            dma((len(LAST) + 2,)),
            *[one] * 3,
        ]
        hbm, vmem = pl.BlockSpec(memory_space=pltpu.HBM), pl.BlockSpec(memory_space=pltpu.VMEM)
        inside = pl.pallas_call(
            body,
            out_shape=[*(pltpu.VMEM(one, jnp.bfloat16) for one in full), *moments, *moments],
            in_specs=[hbm] * len(arrays),
            out_specs=[vmem] * (3 * count),
            scratch_shapes=[*scratch, *semaphores],
            compiler_params=pltpu.CompilerParams(collective_id=0, has_side_effects=True, vmem_limit_bytes=SCRATCH_BYTES),
        )(*arrays)
        shapes = [jax.ShapeDtypeStruct(w.shape, w.dtype) for w in weights] + [jax.ShapeDtypeStruct(b, jnp.float32) for b in blocks] * 2
        return pl.pallas_call(
            functools.partial(write_out, groups, layers),
            out_shape=shapes,
            in_specs=[vmem] * (3 * count),
            out_specs=[hbm] * len(shapes),
            scratch_shapes=[dma((3 * count,))],
            compiler_params=pltpu.CompilerParams(vmem_limit_bytes=WRITE_BYTES),
        )(*inside)

    all_of, shared = P(None, None, None), P(None, "dp", None)
    return jax.shard_map(
        step,
        mesh=mesh,
        in_specs=(P(("rep", "dp"), None, None, None),) * 3 + (all_of,) * 3 + (shared,) * 6,
        out_specs=(P("rep", None, None),) * 3 + (P("rep", "dp", None),) * 6,
        check_vma=False,
    )
```
